64 devices in a mesh: dp: 4 (over x, y), sp: 16 (over z, core).
Axes of the slice: x: 2, y: 2, z: 8, core: 2. Of those that a mesh axis runs over, the one named last changes fastest.
The devices are a block of a 4x4x8 slice.
Arguments:
- prompt: bfloat16 [4, 1024, 4096], P('dp', 'sp'), parts along dimension 0
- w_q: bfloat16 [4096, 4096], replicated
- w_k: bfloat16 [4096, 4096], replicated
- w_v: bfloat16 [4096, 4096], replicated
- w_o: bfloat16 [4096, 4096], replicated
- q_norm_w: float32 [4096], replicated
- k_norm_w: float32 [4096], replicated
- post_norm_w: float32 [4096], replicated
- new_token: bfloat16 [4, 4096], P('dp'), parts along dimension 0
Outputs:
- output 1: bfloat16 [4, 1024, 4096], P('dp', 'sp'), parts along dimension 0
- output 2: bfloat16 [4, 1025, 32, 128], P('dp', None, 'sp'), parts along dimension 0
- output 3: bfloat16 [4, 1025, 32, 128], P('dp', None, 'sp'), parts along dimension 0
- output 4: bfloat16 [4, 4096], P('dp'), parts along dimension 0
There are 4 independent parts. The reference program is written for one: setup_inputs(seed, part) draws one part's arguments, and reference() takes and returns one part's arrays. A program takes and returns all parts, laid end to end along the dimension named above; an argument that names none is the same for every part.
All inputs are finite; a program needn't handle non-finite values.
Results may differ from the reference program's by a relative error of at most 0.00684954.
Values are sent between devices in bfloat16 or wider.
A program may use at most 768 MiB of HBM per device.

```python
import jax
import jax.numpy as jnp
from jax import lax

BATCH_ROWS = 1
TOKENS_DEV = 64
GROUP_SIZE = 16
MODEL_WIDTH = 4096
NUM_HEADS = 32
HEAD_DIM = 128

SEQ_LEN = TOKENS_DEV * GROUP_SIZE
HEADS_LOCAL = NUM_HEADS // GROUP_SIZE
QUERY_ROWS = min(TOKENS_DEV, 128)
ROPE_THETA = 500000.0
NORM_EPS = 1e-6


def setup_inputs(seed: int = 0, part: int = 0) -> dict:
    base_key = jax.random.key(seed)
    part_key = jax.random.fold_in(base_key, part)
    w_keys = jax.random.split(base_key, 9)
    x_keys = jax.random.split(part_key, 2)
    fan_scale = MODEL_WIDTH ** -0.5
    q_heads = jnp.exp(jax.random.uniform(w_keys[0], (NUM_HEADS,), jnp.float32, -0.5, 0.5))
    k_heads = jnp.exp(jax.random.uniform(w_keys[1], (NUM_HEADS,), jnp.float32, -0.5, 0.5))
    q_cols = jnp.repeat(q_heads, HEAD_DIM) * fan_scale
    k_cols = jnp.repeat(k_heads, HEAD_DIM) * fan_scale
    w_shape = (MODEL_WIDTH, MODEL_WIDTH)
    w_q = (jax.random.normal(w_keys[2], w_shape, jnp.float32) * q_cols[None, :]).astype(jnp.bfloat16)
    w_k = (jax.random.normal(w_keys[3], w_shape, jnp.float32) * k_cols[None, :]).astype(jnp.bfloat16)
    w_v = (jax.random.normal(w_keys[4], w_shape, jnp.float32) * fan_scale).astype(jnp.bfloat16)
    w_o = (jax.random.normal(w_keys[5], w_shape, jnp.float32) * fan_scale).astype(jnp.bfloat16)
    q_norm_w = jax.random.uniform(w_keys[6], (MODEL_WIDTH,), jnp.float32, 0.5, 1.5)
    k_norm_w = jax.random.uniform(w_keys[7], (MODEL_WIDTH,), jnp.float32, 0.5, 1.5)
    post_norm_w = jax.random.uniform(w_keys[8], (MODEL_WIDTH,), jnp.float32, 0.5, 1.5)
    prompt = jax.random.normal(x_keys[0], (BATCH_ROWS, SEQ_LEN, MODEL_WIDTH), jnp.float32).astype(jnp.bfloat16)
    new_token = jax.random.normal(x_keys[1], (BATCH_ROWS, MODEL_WIDTH), jnp.float32).astype(jnp.bfloat16)
    return {"prompt": prompt, "w_q": w_q, "w_k": w_k, "w_v": w_v, "w_o": w_o, "q_norm_w": q_norm_w, "k_norm_w": k_norm_w, "post_norm_w": post_norm_w, "new_token": new_token}


def rms_norm(values, weight):
    return values * lax.rsqrt(jnp.mean(values * values, axis=-1, keepdims=True) + NORM_EPS) * weight


def rope_tables(positions):
    inv_freq = ROPE_THETA ** (-jnp.arange(0, HEAD_DIM, 2).astype(jnp.float32) / HEAD_DIM)
    angles = positions.astype(jnp.float32)[:, None] * inv_freq[None, :]
    angles = jnp.concatenate([angles, angles], axis=-1)
    return jnp.cos(angles), jnp.sin(angles)


def apply_rope(values, cos_t, sin_t):
    half_dim = HEAD_DIM // 2
    rotated = jnp.concatenate([-values[..., half_dim:], values[..., :half_dim]], axis=-1)
    return values * cos_t[:, None, :] + rotated * sin_t[:, None, :]


def project_heads(x_rows, w_mat, norm_w, cos_t, sin_t):
    normed = rms_norm(jnp.dot(x_rows, w_mat, preferred_element_type=jnp.float32), norm_w)
    return apply_rope(normed.reshape(x_rows.shape[0], NUM_HEADS, HEAD_DIM), cos_t, sin_t).astype(jnp.bfloat16)


def one_sequence(prompt_seq, new_row, w_q, w_k, w_v, w_o, q_norm_w, k_norm_w, post_norm_w):
    score_scale = HEAD_DIM ** -0.5
    cos_p, sin_p = rope_tables(jnp.arange(SEQ_LEN))
    q_seq = project_heads(prompt_seq, w_q, q_norm_w, cos_p, sin_p)
    k_seq = project_heads(prompt_seq, w_k, k_norm_w, cos_p, sin_p)
    v_seq = jnp.dot(prompt_seq, w_v, preferred_element_type=jnp.float32).astype(jnp.bfloat16).reshape(SEQ_LEN, NUM_HEADS, HEAD_DIM)
    k_wide = k_seq.astype(jnp.float32)
    v_wide = v_seq.astype(jnp.float32)
    key_pos = jnp.arange(SEQ_LEN)

    def query_block(block_idx):
        q_blk = lax.dynamic_slice_in_dim(q_seq, block_idx * QUERY_ROWS, QUERY_ROWS, axis=0).astype(jnp.float32)
        q_pos = block_idx * QUERY_ROWS + jnp.arange(QUERY_ROWS)
        scores = jnp.einsum("qhd,khd->hqk", q_blk, k_wide) * score_scale
        scores = jnp.where((q_pos[:, None] >= key_pos[None, :])[None], scores, -1e30)
        attn_p = jax.nn.softmax(scores, axis=-1).astype(jnp.bfloat16)
        return jnp.einsum("hqk,khd->qhd", attn_p.astype(jnp.float32), v_wide).astype(jnp.bfloat16)

    attn_out = lax.map(query_block, jnp.arange(SEQ_LEN // QUERY_ROWS)).reshape(SEQ_LEN, MODEL_WIDTH)
    proj_pre = jnp.dot(attn_out, w_o, preferred_element_type=jnp.float32)
    out_p = (prompt_seq.astype(jnp.float32) + rms_norm(proj_pre, post_norm_w)).astype(jnp.bfloat16)
    cos_d, sin_d = rope_tables(jnp.full((1,), SEQ_LEN))
    q_new = project_heads(new_row[None, :], w_q, q_norm_w, cos_d, sin_d)[0]
    k_new = project_heads(new_row[None, :], w_k, k_norm_w, cos_d, sin_d)[0]
    v_new = jnp.dot(new_row[None, :], w_v, preferred_element_type=jnp.float32).astype(jnp.bfloat16).reshape(NUM_HEADS, HEAD_DIM)
    k_cache = jnp.concatenate([k_seq, k_new[None]], axis=0)
    v_cache = jnp.concatenate([v_seq, v_new[None]], axis=0)
    scores_d = jnp.einsum("hd,khd->hk", q_new.astype(jnp.float32), k_cache.astype(jnp.float32)) * score_scale
    attn_d = jax.nn.softmax(scores_d, axis=-1).astype(jnp.bfloat16)
    o_new = jnp.einsum("hk,khd->hd", attn_d.astype(jnp.float32), v_cache.astype(jnp.float32)).astype(jnp.bfloat16)
    o_groups = o_new.reshape(GROUP_SIZE, HEADS_LOCAL * HEAD_DIM).astype(jnp.float32)
    w_groups = w_o.reshape(GROUP_SIZE, HEADS_LOCAL * HEAD_DIM, MODEL_WIDTH).astype(jnp.float32)
    part_proj = jnp.einsum("gc,gcn->gn", o_groups, w_groups).astype(jnp.bfloat16)
    proj_new = jnp.sum(part_proj.astype(jnp.float32), axis=0)
    out_d = (new_row.astype(jnp.float32) + rms_norm(proj_new, post_norm_w)).astype(jnp.bfloat16)
    return out_p, k_cache, v_cache, out_d


def reference(prompt, w_q, w_k, w_v, w_o, q_norm_w, k_norm_w, post_norm_w, new_token):
    out_p, k_cache, v_cache, out_d = lax.map(
        lambda seq_pair: one_sequence(seq_pair[0], seq_pair[1], w_q, w_k, w_v, w_o, q_norm_w, k_norm_w, post_norm_w),
        (prompt, new_token))
    return out_p, k_cache, v_cache, out_d
```

```python
import functools
import math

import jax
import jax.numpy as jnp
import numpy as np
from jax import lax
from jax.experimental import pallas as pl
from jax.experimental.pallas import tpu as pltpu
from jax.sharding import PartitionSpec as P

HEAD_DIM = 128
ROPE_THETA = 500000.0
NORM_EPS = 1e-6
PAD = 16
MASKED = -1e30
F32 = jnp.float32
BF16 = jnp.bfloat16
MESH = pl.DeviceIdType.MESH


def rope_table(seq_len):
    half = HEAD_DIM // 2
    inv_freq = np.power(np.float32(ROPE_THETA), -np.arange(0, HEAD_DIM, 2).astype(np.float32) / np.float32(HEAD_DIM)).astype(np.float32)
    pos = np.minimum(np.arange(seq_len + PAD), seq_len).astype(np.float32)
    angles = (pos[:, None] * inv_freq[None, :half]).astype(np.float32)
    return np.concatenate([np.cos(angles), np.sin(angles)], axis=-1).astype(np.float32)


def kernel(n_dev, x_hbm, new_ref, wq, wk, wv, wo, qg_ref, kg_ref, pg_ref, tab_hbm,
           outp_ref, kc_hbm, vc_hbm, outd_ref,
           xs, pool, tab, raw, ssq, ssq_in, send, recv, new, s_ref, p_ref, osend, orecv, dsend, dsum, acc, stage, cache,
           xsem, wsem, wosem, tabsem, xs_s, xs_r, ss_s, ss_r, a_s, a_r, d_s, d_r, o_s, o_r, csem):
    tok = x_hbm.shape[0]
    width = x_hbm.shape[1]
    rows = 2 * tok
    n_chip = n_dev // 2
    half_chip = n_chip // 2
    cols = width // n_dev
    heads = cols // HEAD_DIM
    seq = tok * n_dev
    n_step = n_chip // 2
    n_wo = pool.shape[0]
    wide = 2 * cols

    me = lax.axis_index("sp")
    chip = lax.div(me, 2)
    core = lax.rem(me, 2)
    sibling = 2 * chip + (1 - core)

    def offset_of(idx):
        odd = lax.rem(idx, 2)
        return lax.rem(half_chip + odd + (2 * odd - 1) * lax.div(idx, 2), n_chip)

    def group_col(idx):
        dest = lax.rem(chip + offset_of(idx), n_chip)
        return pl.multiple_of((2 * dest + core) * cols, cols)

    def w_copy(w_ref, s, half):
        return pltpu.make_async_copy(
            w_ref.at[:, pl.ds(group_col(2 * s + half), cols)], pool.at[s, :, pl.ds(half * cols, cols)], wsem.at[s, half])

    def wo_copy(j):
        return pltpu.make_async_copy(wo.at[:, pl.ds(pl.multiple_of(j * wide, wide), wide)], pool.at[j], wosem.at[j])

    my_rows = pl.ds(pl.multiple_of(core * tok, tok), tok)
    x_copy = pltpu.make_async_copy(x_hbm, xs.at[my_rows], xsem)
    x_copy.start()
    for s in range(n_step):
        w_copy(wv, s, 0).start()
        w_copy(wv, s, 1).start()
    tab_a = pltpu.make_async_copy(tab_hbm.at[pl.ds(pl.multiple_of(chip * rows, rows), rows)], tab.at[pl.ds(0, rows)], tabsem.at[0])
    tab_b = pltpu.make_async_copy(tab_hbm.at[pl.ds(seq, PAD)], tab.at[pl.ds(rows, PAD)], tabsem.at[1])
    tab_a.start()
    tab_b.start()

    barrier = pltpu.get_barrier_semaphore()
    for off in range(1, n_dev):
        pl.semaphore_signal(barrier, inc=1, device_id={"sp": lax.rem(me + off, n_dev)}, device_id_type=MESH)
    xs[pl.ds(rows, PAD), :] = jnp.broadcast_to(new_ref[...], (PAD, width))
    x_copy.wait()
    pl.semaphore_wait(barrier, n_dev - 1)

    x_send = pltpu.make_async_remote_copy(
        src_ref=xs.at[my_rows], dst_ref=xs.at[my_rows], send_sem=xs_s, recv_sem=xs_r, device_id={"sp": sibling}, device_id_type=MESH)
    x_send.start()
    x_send.wait_recv()

    own_rows = pl.ds(pl.multiple_of(chip * rows, rows), rows)

    def exchange(t, idx):
        dest = lax.rem(chip + offset_of(idx), n_chip)
        return pltpu.make_async_remote_copy(
            src_ref=send.at[t, idx], dst_ref=recv.at[t, own_rows], send_sem=a_s.at[t, idx], recv_sem=a_r.at[t, idx],
            device_id={"sp": 2 * dest + core}, device_id_type=MESH)

    def emit(t, idx, block):
        @pl.when(idx < n_chip - 1)
        def _():
            send[t, idx] = block[:rows]
            exchange(t, idx).start()

        @pl.when(idx == n_chip - 1)
        def _():
            recv[t, own_rows, :] = block[:rows]
            new[t] = block[rows:]

    def project(s):
        w_copy(wv, s, 0).wait()
        w_copy(wv, s, 1).wait()
        return jnp.dot(xs[...], pool[s], preferred_element_type=F32)

    def v_step(s, carry):
        res = project(s)
        w_copy(wk, s, 0).start()
        w_copy(wk, s, 1).start()
        for half in range(2):
            emit(2, 2 * s + half, res[:, half * cols:(half + 1) * cols].astype(BF16))
        return carry

    lax.fori_loop(0, n_step, v_step, 0)
    tab_a.wait()
    tab_b.wait()

    lane = lax.broadcasted_iota(jnp.int32, (rows + PAD, HEAD_DIM), 1)
    first = lane < HEAD_DIM // 2

    def raw_step(t, s):
        res = project(s)
        sq = jnp.zeros((rows + PAD, HEAD_DIM), F32)
        for half in range(2):
            part = res[:, half * cols:(half + 1) * cols]
            raw[2 * s + half] = part
            for h in range(heads):
                piece = part[:, h * HEAD_DIM:(h + 1) * HEAD_DIM]
                sq = sq + piece * piece
        @pl.when(s == 0)
        def _():
            ssq[t] = sq

        @pl.when(s > 0)
        def _():
            ssq[t] += sq

    def norm_and_send(t, g_ref):
        swap = pltpu.make_async_remote_copy(
            src_ref=ssq.at[t], dst_ref=ssq_in.at[t], send_sem=ss_s.at[t], recv_sem=ss_r.at[t],
            device_id={"sp": sibling}, device_id_type=MESH)
        swap.start()
        swap.wait_recv()
        total = jnp.sum(ssq[t] + ssq_in[t], axis=1, keepdims=True)
        scale = lax.rsqrt(total * (1.0 / width) + NORM_EPS)

        def one(idx, carry):
            g = g_ref[:, pl.ds(group_col(idx), cols)]
            table = tab[...]
            turned = pltpu.roll(table, HEAD_DIM // 2, 1)
            cos = jnp.where(first, table, turned)
            sin = jnp.where(first, -turned, table)
            parts = []
            for h in range(heads):
                at = slice(h * HEAD_DIM, (h + 1) * HEAD_DIM)
                val = raw[idx, :, at] * scale * g[:, at]
                parts.append((val * cos + pltpu.roll(val, HEAD_DIM // 2, 1) * sin).astype(BF16))
            emit(t, idx, jnp.concatenate(parts, axis=1))
            return carry

        lax.fori_loop(0, n_chip, one, 0)

    def k_step(s, carry):
        raw_step(1, s)
        w_copy(wq, s, 0).start()
        w_copy(wq, s, 1).start()
        return carry

    lax.fori_loop(0, n_step, k_step, 0)
    norm_and_send(1, kg_ref)
    for j in range(n_step, n_wo):
        wo_copy(j).start()

    def q_step(s, carry):
        raw_step(0, s)
        wo_copy(s).start()
        return carry

    lax.fori_loop(0, n_step, q_step, 0)
    norm_and_send(0, qg_ref)

    def arrivals(t):
        def one(idx, carry):
            exchange(t, idx).wait_recv()
            return carry
        lax.fori_loop(0, n_chip - 1, one, 0)

    def fill_cache(t, which, out_hbm):
        def one(b, carry):
            base = pl.multiple_of(b * rows, rows)
            block = recv[t, pl.ds(base, rows), :].astype(F32)
            for h in range(heads):
                stage[pl.ds(h, rows, stride=heads), :] = block[:, h * HEAD_DIM:(h + 1) * HEAD_DIM]
            cache[which, pl.ds(pl.multiple_of(heads * base, heads * rows), heads * rows), :] = stage[...].astype(BF16)
            return carry
        lax.fori_loop(0, n_chip, one, 0)
        last = new[t][0:1, :].astype(F32)
        rows_new = jnp.concatenate([last[:, h * HEAD_DIM:(h + 1) * HEAD_DIM] for h in range(heads)], axis=0)
        cache[which, pl.ds(heads * seq, heads), :] = rows_new.astype(BF16)
        pltpu.make_async_copy(cache.at[which], out_hbm, csem.at[which]).start()

    arrivals(2)
    fill_cache(2, 1, vc_hbm)
    arrivals(1)
    fill_cache(1, 0, kc_hbm)

    log_scale = HEAD_DIM ** -0.5 * math.log2(math.e)
    contract_last = (((1,), (1,)), ((), ()))

    for h in range(heads):
        at = slice(h * HEAD_DIM, (h + 1) * HEAD_DIM)
        qd, kd, vd = new[0][:, at], new[1][:, at], new[2][:, at]
        sc = lax.dot_general(qd, recv[1, :, at], contract_last, preferred_element_type=F32) * log_scale
        sn = jnp.sum(qd.astype(F32) * kd.astype(F32), axis=1, keepdims=True) * log_scale
        top = jnp.maximum(jnp.max(sc, axis=1, keepdims=True), sn)
        ex = jnp.exp2(sc - top)
        en = jnp.exp2(sn - top)
        inv = 1.0 / (jnp.sum(ex, axis=1, keepdims=True) + en)
        prob = (ex * inv).astype(BF16)
        prob_n = (en * inv).astype(BF16).astype(F32)
        od = jnp.dot(prob, recv[2, :, at], preferred_element_type=F32) + prob_n * vd.astype(F32)
        dsend[:, at] = od[0:1].astype(BF16).astype(F32)

    def d_copy(off, kk, to):
        return pltpu.make_async_remote_copy(
            src_ref=dsend, dst_ref=dsum.at[2 * off + core], send_sem=d_s.at[off, kk], recv_sem=d_r.at[off, core],
            device_id={"sp": to}, device_id_type=MESH)

    d_copy(0, 0, sibling).start()
    for off in range(1, n_chip):
        for kk in range(2):
            d_copy(off, kk, 2 * lax.rem(chip + off, n_chip) + kk).start()
    dsum[core] = dsend[...]

    def o_copy(i, kk, to, off_o):
        return pltpu.make_async_remote_copy(
            src_ref=osend.at[i, pl.ds(pl.multiple_of(kk * tok, tok), tok)],
            dst_ref=orecv.at[off_o, pl.ds(0, tok), pl.ds(pl.multiple_of(core * cols, cols), cols)],
            send_sem=o_s.at[i, kk], recv_sem=o_r.at[off_o, core], device_id={"sp": to}, device_id_type=MESH)

    def attend(i, carry):
        idx = lax.rem(i + n_chip - 1, n_chip)
        off_q = offset_of(idx)
        src = lax.rem(chip + n_chip - off_q, n_chip)
        off_o = lax.rem(n_chip - off_q, n_chip)

        @pl.when(i > 0)
        def _():
            exchange(0, idx).wait_recv()

        q_at = pl.ds(pl.multiple_of(src * rows, rows), rows)
        for h in range(heads):
            at = slice(h * HEAD_DIM, (h + 1) * HEAD_DIM)
            s_ref[...] = lax.dot_general(recv[0, q_at, at], recv[1, :, at], contract_last, preferred_element_type=F32)

            def soft(r, c):
                r_at = pl.ds(pl.multiple_of(r * PAD, PAD), PAD)
                sc = s_ref[r_at, :] * log_scale
                q_pos = src * rows + r * PAD + lax.broadcasted_iota(jnp.int32, sc.shape, 0)
                sc = jnp.where(q_pos >= lax.broadcasted_iota(jnp.int32, sc.shape, 1), sc, MASKED)
                ex = jnp.exp2(sc - jnp.max(sc, axis=1, keepdims=True))
                inv = 1.0 / jnp.sum(ex, axis=1, keepdims=True)
                p_ref[r_at, :] = (ex * inv).astype(BF16)
                return c

            lax.fori_loop(0, rows // PAD, soft, 0)
            osend[i, :, at] = jnp.dot(p_ref[...], recv[2, :, at], preferred_element_type=F32).astype(BF16)

        @pl.when(i > 0)
        def _():
            for kk in range(2):
                o_copy(i, kk, 2 * src + kk, off_o).start()

        @pl.when(i == 0)
        def _():
            o_copy(i, 1 - core, sibling, off_o).start()
            orecv[0, pl.ds(0, tok), pl.ds(pl.multiple_of(core * cols, cols), cols)] = osend[0, my_rows, :]
        return carry

    lax.fori_loop(0, n_chip, attend, 0)

    for j in range(n_wo):
        wo_copy(j).wait()

    zero_half = jnp.zeros((8, cols), BF16)

    def gather(i, carry):
        off_o = lax.rem(n_chip - offset_of(lax.rem(i + n_chip - 1, n_chip)), n_chip)
        src = lax.rem(chip + n_chip - off_o, n_chip)

        def wait_pair(kk):
            pltpu.make_async_remote_copy(
                src_ref=osend.at[0, pl.ds(0, tok)], dst_ref=orecv.at[off_o, pl.ds(0, tok), pl.ds(pl.multiple_of(kk * cols, cols), cols)],
                send_sem=o_s.at[0, 0], recv_sem=o_r.at[off_o, kk], device_id={"sp": sibling}, device_id_type=MESH).wait_recv()
            pltpu.make_async_remote_copy(
                src_ref=dsend, dst_ref=dsum.at[2 * off_o + kk], send_sem=d_s.at[0, 0], recv_sem=d_r.at[off_o, kk],
                device_id={"sp": sibling}, device_id_type=MESH).wait_recv()

        @pl.when(i == 0)
        def _():
            wait_pair(1 - core)

        @pl.when(i > 0)
        def _():
            wait_pair(0)
            wait_pair(1)

        d0 = jnp.broadcast_to(dsum[2 * off_o].astype(BF16), (8, cols))
        d1 = jnp.broadcast_to(dsum[2 * off_o + 1].astype(BF16), (8, cols))
        orecv[off_o, pl.ds(tok, PAD), :] = jnp.concatenate(
            [jnp.concatenate([d0, zero_half], axis=1), jnp.concatenate([zero_half, d1], axis=1)], axis=0)
        k_at = pl.ds(pl.multiple_of(src * wide, wide), wide)
        lhs = orecv[off_o]
        for j in range(n_wo):
            res = jnp.dot(lhs, pool[j, k_at, :], preferred_element_type=F32)
            parts = res[tok:tok + 8].astype(BF16).astype(F32) + res[tok + 8:].astype(BF16).astype(F32)
            n_at = slice(j * wide, (j + 1) * wide)

            @pl.when(i == 0)
            def _():
                acc[pl.ds(0, tok), n_at] = res[:tok]
                acc[pl.ds(tok, 8), n_at] = parts

            @pl.when(i > 0)
            def _():
                acc[pl.ds(0, tok), n_at] += res[:tok]
                acc[pl.ds(tok, 8), n_at] += parts
        return carry

    lax.fori_loop(0, n_chip, gather, 0)

    def finish(r, carry):
        r_at = pl.ds(pl.multiple_of(r * PAD, PAD), PAD)
        val = acc[r_at, :]
        scale = lax.rsqrt(jnp.sum(val * val, axis=1, keepdims=True) * (1.0 / width) + NORM_EPS)
        x_at = pl.ds(pl.multiple_of(core * tok + r * PAD, PAD), PAD)
        outp_ref[r_at, :] = (xs[x_at, :].astype(F32) + val * scale * pg_ref[...]).astype(BF16)
        return carry

    lax.fori_loop(0, tok // PAD, finish, 0)
    val = acc[pl.ds(tok, 8), :]
    scale = lax.rsqrt(jnp.sum(val * val, axis=1, keepdims=True) * (1.0 / width) + NORM_EPS)
    outd_ref[...] = (new_ref[...].astype(F32) + (val * scale * pg_ref[...])[0:1]).astype(BF16)

    x_send.wait_send()
    for t in range(2):
        pltpu.make_async_remote_copy(
            src_ref=ssq.at[t], dst_ref=ssq_in.at[t], send_sem=ss_s.at[t], recv_sem=ss_r.at[t],
            device_id={"sp": sibling}, device_id_type=MESH).wait_send()

    def drain(idx, carry):
        for t in range(3):
            exchange(t, idx).wait_send()
        for kk in range(2):
            o_copy(idx + 1, kk, sibling, 0).wait_send()
            d_copy(idx + 1, kk, sibling).wait_send()
        return carry

    lax.fori_loop(0, n_chip - 1, drain, 0)
    o_copy(0, 1 - core, sibling, 0).wait_send()
    d_copy(0, 0, sibling).wait_send()
    pltpu.make_async_copy(cache.at[1], vc_hbm, csem.at[1]).wait()
    pltpu.make_async_copy(cache.at[0], kc_hbm, csem.at[0]).wait()


def solution(mesh):
    n_dev = mesh.shape["sp"]

    def device_step(prompt_blk, w_q, w_k, w_v, w_o, q_norm_w, k_norm_w, post_norm_w, new_rows):
        _, tok, width = prompt_blk.shape
        n_chip = n_dev // 2
        rows, seq, cols = 2 * tok, tok * n_dev, width // n_dev
        heads = cols // HEAD_DIM
        wide = 2 * cols
        n_wo = width // wide
        table = jnp.asarray(rope_table(seq))
        vmem = pl.BlockSpec(memory_space=pltpu.VMEM)
        hbm = pl.BlockSpec(memory_space=pl.ANY)
        dma = pltpu.SemaphoreType.DMA
        cache_shape = jax.ShapeDtypeStruct((heads * (seq + 1), HEAD_DIM), BF16)
        outp, kc, vc, outd = pl.pallas_call(
            functools.partial(kernel, n_dev),
            out_shape=(jax.ShapeDtypeStruct((tok, width), BF16), cache_shape, cache_shape, jax.ShapeDtypeStruct((1, width), BF16)),
            in_specs=[hbm, vmem, hbm, hbm, hbm, hbm, vmem, vmem, vmem, hbm],
            out_specs=(vmem, hbm, hbm, vmem),
            scratch_shapes=[
                pltpu.VMEM((rows + PAD, width), BF16),
                pltpu.VMEM((n_wo, width, wide), BF16),
                pltpu.VMEM((rows + PAD, HEAD_DIM), F32),
                pltpu.VMEM((n_chip, rows + PAD, cols), F32),
                pltpu.VMEM((2, rows + PAD, HEAD_DIM), F32),
                pltpu.VMEM((2, rows + PAD, HEAD_DIM), F32),
                pltpu.VMEM((3, n_chip, rows, cols), BF16),
                pltpu.VMEM((3, seq, cols), BF16),
                pltpu.VMEM((3, PAD, cols), BF16),
                pltpu.VMEM((rows, seq), F32),
                pltpu.VMEM((rows, seq), BF16),
                pltpu.VMEM((n_chip, rows, cols), BF16),
                pltpu.VMEM((n_chip, tok + PAD, wide), BF16),
                pltpu.VMEM((1, cols), F32),
                pltpu.VMEM((n_dev, 1, cols), F32),
                pltpu.VMEM((tok + 8, width), F32),
                pltpu.VMEM((heads * rows, HEAD_DIM), F32),
                pltpu.VMEM((2, heads * (seq + 1), HEAD_DIM), BF16),
                dma(()), dma((n_chip // 2, 2)), dma((n_wo,)), dma((2,)),
                dma(()), dma(()), dma((2,)), dma((2,)),
                dma((3, n_chip)), dma((3, n_chip)),
                dma((n_chip, 2)), dma((n_chip, 2)),
                dma((n_chip, 2)), dma((n_chip, 2)),
                dma((2,)),
            ],
            compiler_params=pltpu.CompilerParams(collective_id=0, has_side_effects=True, vmem_limit_bytes=62 * 1024 * 1024),
        )(prompt_blk[0], new_rows, w_q, w_k, w_v, w_o, q_norm_w[None], k_norm_w[None], post_norm_w[None], table)
        shape = (1, seq + 1, heads, HEAD_DIM)
        return outp[None], kc.reshape(shape), vc.reshape(shape), outd

    replicated = P()
    return jax.shard_map(
        device_step, mesh=mesh,
        in_specs=(P("dp", "sp", None), replicated, replicated, replicated, replicated, replicated, replicated, replicated, P("dp", None)),
        out_specs=(P("dp", "sp", None), P("dp", None, "sp", None), P("dp", None, "sp", None), P("dp", None)),
        check_vma=False)
```

```python
import functools
import math

import jax
import jax.numpy as jnp
import numpy as np
from jax import lax
from jax.experimental import pallas as pl
from jax.experimental.pallas import tpu as pltpu
from jax.sharding import PartitionSpec as P

HEAD_DIM = 128
ROPE_THETA = 500000.0
NORM_EPS = 1e-6
PAD = 16
LAG = 4
MASKED = -1e30
F32 = jnp.float32
BF16 = jnp.bfloat16
MESH = pl.DeviceIdType.MESH


def rope_table(seq_len):
    half = HEAD_DIM // 2
    inv_freq = np.power(np.float32(ROPE_THETA), -np.arange(0, HEAD_DIM, 2).astype(np.float32) / np.float32(HEAD_DIM)).astype(np.float32)
    pos = np.minimum(np.arange(seq_len + PAD), seq_len).astype(np.float32)
    angles = (pos[:, None] * inv_freq[None, :half]).astype(np.float32)
    return np.concatenate([np.cos(angles), np.sin(angles)], axis=-1).astype(np.float32)


def kernel(n_dev, x_hbm, new_hbm, wq, wk, wv, wo, qg_hbm, kg_hbm, pg_hbm, tab_hbm,
           outp_hbm, kc_hbm, vc_hbm, outd_hbm,
           new_ref, qg_ref, kg_ref, pg_ref, outp_ref, outd_ref,
           xs, pool, tab, raw, ssq, ssq_in, send, recv, new, s_ref, p_ref, vt, osend, orecv, dsend, dsum, acc, stage, cache,
           xsem, insem, outsem, wsem, wosem, tabsem, xs_s, xs_r, ss_s, ss_r, a_s, a_r, d_s, d_r, o_s, o_r, csem):
    tok = x_hbm.shape[0]
    width = x_hbm.shape[1]
    rows = 2 * tok
    n_chip = n_dev // 2
    half_chip = n_chip // 2
    cols = width // n_dev
    heads = cols // HEAD_DIM
    seq = tok * n_dev
    n_step = n_chip // 2
    n_wo = pool.shape[0]
    wide = 2 * cols

    me = lax.axis_index("sp")
    chip = lax.div(me, 2)
    core = lax.rem(me, 2)
    sibling = 2 * chip + (1 - core)

    def offset_of(idx):
        odd = lax.rem(idx, 2)
        return lax.rem(half_chip + odd + (2 * odd - 1) * lax.div(idx, 2), n_chip)

    def group_col(idx):
        dest = lax.rem(chip + offset_of(idx), n_chip)
        return pl.multiple_of((2 * dest + core) * cols, cols)

    def w_copy(w_ref, s, half):
        return pltpu.make_async_copy(
            w_ref.at[:, pl.ds(group_col(2 * s + half), cols)], pool.at[s, :, pl.ds(half * cols, cols)], wsem.at[s, half])

    def wo_copy(j):
        return pltpu.make_async_copy(wo.at[:, pl.ds(pl.multiple_of(j * wide, wide), wide)], pool.at[j], wosem.at[j])

    my_rows = pl.ds(pl.multiple_of(core * tok, tok), tok)
    x_copy = pltpu.make_async_copy(x_hbm, xs.at[my_rows], xsem)
    x_copy.start()
    smalls = [pltpu.make_async_copy(a, b, insem.at[n]) for n, (a, b) in enumerate(
        ((new_hbm, new_ref), (qg_hbm, qg_ref), (kg_hbm, kg_ref), (pg_hbm, pg_ref)))]
    for small in smalls:
        small.start()
    tab_a = pltpu.make_async_copy(tab_hbm.at[pl.ds(pl.multiple_of(chip * rows, rows), rows)], tab.at[pl.ds(0, rows)], tabsem.at[0])
    tab_b = pltpu.make_async_copy(tab_hbm.at[pl.ds(seq, PAD)], tab.at[pl.ds(rows, PAD)], tabsem.at[1])
    tab_a.start()
    tab_b.start()

    barrier = pltpu.get_barrier_semaphore()
    for off in range(1, n_dev):
        pl.semaphore_signal(barrier, inc=1, device_id={"sp": lax.rem(me + off, n_dev)}, device_id_type=MESH)
    for small in smalls:
        small.wait()
    x_copy.wait()
    for s in range(n_step):
        w_copy(wv, s, 0).start()
        w_copy(wv, s, 1).start()
    xs[pl.ds(rows, PAD), :] = jnp.broadcast_to(new_ref[...], (PAD, width))
    with jax.named_scope("barrier"):
        pl.semaphore_wait(barrier, n_dev - 1)

    x_send = pltpu.make_async_remote_copy(
        src_ref=xs.at[my_rows], dst_ref=xs.at[my_rows], send_sem=xs_s, recv_sem=xs_r, device_id={"sp": sibling}, device_id_type=MESH)
    x_send.start()
    acc[...] = jnp.zeros_like(acc)
    with jax.named_scope('x_arrive'):
        x_send.wait_recv()

    own_rows = pl.ds(pl.multiple_of(chip * rows, rows), rows)

    def exchange(t, idx):
        dest = lax.rem(chip + offset_of(idx), n_chip)
        return pltpu.make_async_remote_copy(
            src_ref=send.at[t, idx], dst_ref=recv.at[t, own_rows], send_sem=a_s.at[t, idx], recv_sem=a_r.at[t, idx],
            device_id={"sp": 2 * dest + core}, device_id_type=MESH)

    def emit(t, idx, block):
        @pl.when(idx < n_chip - 1)
        def _():
            send[t, idx] = block[:rows]
            exchange(t, idx).start()

        @pl.when(idx == n_chip - 1)
        def _():
            recv[t, own_rows, :] = block[:rows]
            new[t] = block[rows:]

    def project(s):
        w_copy(wv, s, 0).wait()
        w_copy(wv, s, 1).wait()
        return jnp.dot(xs[...], pool[s], preferred_element_type=F32)

    def v_step(s, carry):
        res = project(s)
        w_copy(wk, s, 0).start()
        w_copy(wk, s, 1).start()
        for half in range(2):
            emit(2, 2 * s + half, res[:, half * cols:(half + 1) * cols].astype(BF16))
        return carry

    with jax.named_scope('v_proj'):
        lax.fori_loop(0, n_step, v_step, 0)
    tab_a.wait()
    tab_b.wait()

    lane = lax.broadcasted_iota(jnp.int32, (rows + PAD, HEAD_DIM), 1)
    first = lane < HEAD_DIM // 2

    def raw_step(t, s):
        res = project(s)
        sq = jnp.zeros((rows + PAD, HEAD_DIM), F32)
        for half in range(2):
            part = res[:, half * cols:(half + 1) * cols]
            raw[2 * s + half] = part
            for h in range(heads):
                piece = part[:, h * HEAD_DIM:(h + 1) * HEAD_DIM]
                sq = sq + piece * piece
        @pl.when(s == 0)
        def _():
            ssq[t] = sq

        @pl.when(s > 0)
        def _():
            ssq[t] += sq

    def norm_and_send(t, g_ref):
        swap = pltpu.make_async_remote_copy(
            src_ref=ssq.at[t], dst_ref=ssq_in.at[t], send_sem=ss_s.at[t], recv_sem=ss_r.at[t],
            device_id={"sp": sibling}, device_id_type=MESH)
        swap.start()
        swap.wait_recv()
        total = jnp.sum(ssq[t] + ssq_in[t], axis=1, keepdims=True)
        scale = lax.rsqrt(total * (1.0 / width) + NORM_EPS)

        def one(idx, carry):
            g = g_ref[:, pl.ds(group_col(idx), cols)]
            table = tab[...]
            turned = pltpu.roll(table, HEAD_DIM // 2, 1)
            cos = jnp.where(first, table, turned)
            sin = jnp.where(first, -turned, table)
            parts = []
            for h in range(heads):
                at = slice(h * HEAD_DIM, (h + 1) * HEAD_DIM)
                val = raw[idx, :, at] * scale * g[:, at]
                parts.append((val * cos + pltpu.roll(val, HEAD_DIM // 2, 1) * sin).astype(BF16))
            emit(t, idx, jnp.concatenate(parts, axis=1))
            return carry

        lax.fori_loop(0, n_chip, one, 0)

    def k_step(s, carry):
        raw_step(1, s)
        w_copy(wq, s, 0).start()
        w_copy(wq, s, 1).start()
        return carry

    with jax.named_scope('k_proj'):
        lax.fori_loop(0, n_step, k_step, 0)
    with jax.named_scope('k_norm'):
        norm_and_send(1, kg_ref)
    for j in range(n_step, n_wo):
        wo_copy(j).start()

    def q_step(s, carry):
        raw_step(0, s)
        wo_copy(s).start()
        return carry

    with jax.named_scope('q_proj'):
        lax.fori_loop(0, n_step, q_step, 0)
    with jax.named_scope('q_norm'):
        norm_and_send(0, qg_ref)

    def arrivals(t):
        def one(idx, carry):
            exchange(t, idx).wait_recv()
            return carry
        lax.fori_loop(0, n_chip - 1, one, 0)

    def fill_cache(t, which, out_hbm):
        def one(b, carry):
            base = pl.multiple_of(b * rows, rows)
            block = recv[t, pl.ds(base, rows), :].astype(F32)
            for h in range(heads):
                stage[pl.ds(h, rows, stride=heads), :] = block[:, h * HEAD_DIM:(h + 1) * HEAD_DIM]
            cache[which, pl.ds(pl.multiple_of(heads * base, heads * rows), heads * rows), :] = stage[...].astype(BF16)
            return carry
        lax.fori_loop(0, n_chip, one, 0)
        last = new[t][0:1, :].astype(F32)
        rows_new = jnp.concatenate([last[:, h * HEAD_DIM:(h + 1) * HEAD_DIM] for h in range(heads)], axis=0)
        cache[which, pl.ds(heads * seq, heads), :] = rows_new.astype(BF16)
        pltpu.make_async_copy(cache.at[which], out_hbm, csem.at[which]).start()

    with jax.named_scope("v_arrive"):
        arrivals(2)
    with jax.named_scope("v_cache"):
        fill_cache(2, 1, vc_hbm)
        for b in range(n_chip):
            for h in range(heads):
                vt[h, :, b * rows:(b + 1) * rows] = recv[2, b * rows:(b + 1) * rows, h * HEAD_DIM:(h + 1) * HEAD_DIM].astype(F32).T.astype(BF16)
    with jax.named_scope("k_arrive"):
        arrivals(1)
    with jax.named_scope("k_cache"):
        fill_cache(1, 0, kc_hbm)

    log_scale = HEAD_DIM ** -0.5 * math.log2(math.e)
    contract_last = (((1,), (1,)), ((), ()))

    for h in range(heads):
        at = slice(h * HEAD_DIM, (h + 1) * HEAD_DIM)
        qd, kd, vd = new[0][:, at], new[1][:, at], new[2][:, at]
        sc = lax.dot_general(qd, recv[1, :, at], contract_last, preferred_element_type=F32) * log_scale
        sn = jnp.sum(qd.astype(F32) * kd.astype(F32), axis=1, keepdims=True) * log_scale
        top = jnp.maximum(jnp.max(sc, axis=1, keepdims=True), sn)
        ex = jnp.exp2(sc - top)
        en = jnp.exp2(sn - top)
        inv = 1.0 / (jnp.sum(ex, axis=1, keepdims=True) + en)
        prob = (ex * inv).astype(BF16)
        prob_n = (en * inv).astype(BF16).astype(F32)
        od = jnp.dot(prob, recv[2, :, at], preferred_element_type=F32) + prob_n * vd.astype(F32)
        dsend[:, at] = od[0:1].astype(BF16).astype(F32)

    def d_copy(off, kk, to):
        return pltpu.make_async_remote_copy(
            src_ref=dsend, dst_ref=dsum.at[2 * off + core], send_sem=d_s.at[off, kk], recv_sem=d_r.at[off, core],
            device_id={"sp": to}, device_id_type=MESH)

    d_copy(0, 0, sibling).start()
    for off in range(1, n_chip):
        for kk in range(2):
            d_copy(off, kk, 2 * lax.rem(chip + off, n_chip) + kk).start()
    dsum[core] = dsend[...]

    def o_copy(i, kk, to, off_o):
        return pltpu.make_async_remote_copy(
            src_ref=osend.at[i, pl.ds(pl.multiple_of(kk * tok, tok), tok)],
            dst_ref=orecv.at[off_o, pl.ds(0, tok), pl.ds(pl.multiple_of(core * cols, cols), cols)],
            send_sem=o_s.at[i, kk], recv_sem=o_r.at[off_o, core], device_id={"sp": to}, device_id_type=MESH)

    def fold(block, op):
        return op(block.reshape(block.shape[0] // 8, 8, block.shape[1]), axis=0)

    def attend(i):
        idx = lax.rem(i + n_chip - 1, n_chip)
        off_q = offset_of(idx)
        src = lax.rem(chip + n_chip - off_q, n_chip)
        off_o = lax.rem(n_chip - off_q, n_chip)

        @pl.when(i > 0)
        def _():
            with jax.named_scope("q_arrive"):
                exchange(0, idx).wait_recv()

        src_at = pl.ds(pl.multiple_of(src * rows, rows), rows)
        causal = lax.broadcasted_iota(jnp.int32, (rows, rows), 0) <= lax.broadcasted_iota(jnp.int32, (rows, rows), 1)
        blocks = [slice(kb * rows, (kb + 1) * rows) for kb in range(n_chip)]
        tops = []
        for h in range(heads):
            at = slice(h * HEAD_DIM, (h + 1) * HEAD_DIM)
            sc = lax.dot_general(recv[1, :, at], recv[0, src_at, at], contract_last, preferred_element_type=F32)
            s_ref[h] = sc
            top = jnp.full((8, rows), -jnp.inf, F32)
            for kb in range(n_chip):
                top = jnp.maximum(top, fold(sc[blocks[kb]], jnp.max) + jnp.where(kb < src, 0.0, -jnp.inf))
            tops.append(top)
        for h in range(heads):
            at = slice(h * HEAD_DIM, (h + 1) * HEAD_DIM)
            own = jnp.where(causal, s_ref[h, src_at, :], -jnp.inf)
            s_ref[h, src_at, :] = own
            top = jnp.max(jnp.maximum(tops[h], fold(own, jnp.max)), axis=0, keepdims=True) * log_scale
            total = jnp.zeros((8, rows), F32)
            for kb in range(n_chip):
                ex = jnp.exp2(s_ref[h, blocks[kb], :] * log_scale + (jnp.where(kb <= src, 0.0, -jnp.inf) - top))
                s_ref[h, blocks[kb], :] = ex
                total = total + fold(ex, jnp.sum)
            inv = 1.0 / jnp.sum(total, axis=0, keepdims=True)
            for kb in range(n_chip):
                p_ref[h, blocks[kb], :] = (s_ref[h, blocks[kb], :] * inv).astype(BF16)
            osend[i, :, at] = jnp.dot(vt[h], p_ref[h], preferred_element_type=F32).T.astype(BF16)

        @pl.when(i > 0)
        def _():
            for kk in range(2):
                o_copy(i, kk, 2 * src + kk, off_o).start()

        @pl.when(i == 0)
        def _():
            o_copy(i, 1 - core, sibling, off_o).start()
            orecv[0, pl.ds(0, tok), pl.ds(pl.multiple_of(core * cols, cols), cols)] = osend[0, my_rows, :]

    zero_half = jnp.zeros((8, cols), BF16)

    def gather(i):
        off_o = lax.rem(n_chip - offset_of(lax.rem(i + n_chip - 1, n_chip)), n_chip)
        src = lax.rem(chip + n_chip - off_o, n_chip)

        def wait_pair(kk):
            pltpu.make_async_remote_copy(
                src_ref=osend.at[0, pl.ds(0, tok)], dst_ref=orecv.at[off_o, pl.ds(0, tok), pl.ds(pl.multiple_of(kk * cols, cols), cols)],
                send_sem=o_s.at[0, 0], recv_sem=o_r.at[off_o, kk], device_id={"sp": sibling}, device_id_type=MESH).wait_recv()
            pltpu.make_async_remote_copy(
                src_ref=dsend, dst_ref=dsum.at[2 * off_o + kk], send_sem=d_s.at[0, 0], recv_sem=d_r.at[off_o, kk],
                device_id={"sp": sibling}, device_id_type=MESH).wait_recv()

        @pl.when(i == 0)
        def _():
            wait_pair(1 - core)

        @pl.when(i > 0)
        def _():
            with jax.named_scope("o_arrive"):
                wait_pair(0)
                wait_pair(1)

        d0 = jnp.broadcast_to(dsum[2 * off_o].astype(BF16), (8, cols))
        d1 = jnp.broadcast_to(dsum[2 * off_o + 1].astype(BF16), (8, cols))
        orecv[off_o, pl.ds(tok, PAD), :] = jnp.concatenate(
            [jnp.concatenate([d0, zero_half], axis=1), jnp.concatenate([zero_half, d1], axis=1)], axis=0)
        k_at = pl.ds(pl.multiple_of(src * wide, wide), wide)
        lhs = orecv[off_o]
        for j in range(n_wo):
            res = jnp.dot(lhs, pool[j, k_at, :], preferred_element_type=F32)
            parts = res[tok:tok + 8].astype(BF16).astype(F32) + res[tok + 8:].astype(BF16).astype(F32)
            n_at = slice(j * wide, (j + 1) * wide)
            acc[pl.ds(0, tok), n_at] += res[:tok]
            acc[pl.ds(tok, 8), n_at] += parts

    def both(i, carry):
        @pl.when(i < n_chip)
        def _():
            with jax.named_scope("attend"):
                attend(i)

        @pl.when(i == LAG)
        def _():
            for j in range(n_wo):
                wo_copy(j).wait()

        @pl.when(i >= LAG)
        def _():
            with jax.named_scope("gather"):
                gather(i - LAG)
        return carry

    lax.fori_loop(0, n_chip + LAG, both, 0)

    def outp_copy(r):
        r_at = pl.ds(pl.multiple_of(r * PAD, PAD), PAD)
        return pltpu.make_async_copy(outp_ref.at[r_at], outp_hbm.at[r_at], outsem.at[r])

    def finish(r, carry):
        r_at = pl.ds(pl.multiple_of(r * PAD, PAD), PAD)
        val = acc[r_at, :]
        scale = lax.rsqrt(jnp.sum(val * val, axis=1, keepdims=True) * (1.0 / width) + NORM_EPS)
        x_at = pl.ds(pl.multiple_of(core * tok + r * PAD, PAD), PAD)
        outp_ref[r_at, :] = (xs[x_at, :].astype(F32) + val * scale * pg_ref[...]).astype(BF16)
        outp_copy(r).start()
        return carry

    with jax.named_scope("finish"):
        lax.fori_loop(0, tok // PAD, finish, 0)
        val = acc[pl.ds(tok, 8), :]
        scale = lax.rsqrt(jnp.sum(val * val, axis=1, keepdims=True) * (1.0 / width) + NORM_EPS)
        outd_ref[...] = (new_ref[...].astype(F32) + (val * scale * pg_ref[...])[0:1]).astype(BF16)
        outd_copy = pltpu.make_async_copy(outd_ref, outd_hbm, insem.at[0])
        outd_copy.start()

    x_send.wait_send()
    for t in range(2):
        pltpu.make_async_remote_copy(
            src_ref=ssq.at[t], dst_ref=ssq_in.at[t], send_sem=ss_s.at[t], recv_sem=ss_r.at[t],
            device_id={"sp": sibling}, device_id_type=MESH).wait_send()

    def drain(idx, carry):
        for t in range(3):
            exchange(t, idx).wait_send()
        for kk in range(2):
            o_copy(idx + 1, kk, sibling, 0).wait_send()
            d_copy(idx + 1, kk, sibling).wait_send()
        return carry

    lax.fori_loop(0, n_chip - 1, drain, 0)
    o_copy(0, 1 - core, sibling, 0).wait_send()
    d_copy(0, 0, sibling).wait_send()
    pltpu.make_async_copy(cache.at[1], vc_hbm, csem.at[1]).wait()
    pltpu.make_async_copy(cache.at[0], kc_hbm, csem.at[0]).wait()
    for r in range(tok // PAD):
        outp_copy(r).wait()
    outd_copy.wait()


def hand_over(outp_in, kc_in, vc_in, outd_in, outp, kc, vc, outd, b0, b1, b2, b3, sem):
    ins = [pltpu.make_async_copy(a, b, sem.at[0, n]) for n, (a, b) in enumerate(
        ((outp_in, b0), (kc_in, b1), (vc_in, b2), (outd_in, b3)))]
    outs = [pltpu.make_async_copy(a, b, sem.at[1, n]) for n, (a, b) in enumerate(
        ((b0, outp), (b1, kc.reshape(b1.shape)), (b2, vc.reshape(b2.shape)), (b3, outd)))]
    for one in ins:
        one.start()
    for a, b in zip(ins, outs):
        a.wait()
        b.start()
    for one in outs:
        one.wait()


def solution(mesh):
    n_dev = mesh.shape["sp"]

    def device_step(prompt_blk, w_q, w_k, w_v, w_o, q_norm_w, k_norm_w, post_norm_w, new_rows):
        _, tok, width = prompt_blk.shape
        n_chip = n_dev // 2
        rows, seq, cols = 2 * tok, tok * n_dev, width // n_dev
        heads = cols // HEAD_DIM
        wide = 2 * cols
        n_wo = width // wide
        table = jnp.asarray(rope_table(seq))
        hbm = pl.BlockSpec(memory_space=pl.ANY)
        dma = pltpu.SemaphoreType.DMA
        cache_shape = jax.ShapeDtypeStruct((heads * (seq + 1), HEAD_DIM), BF16)
        outp, kc, vc, outd = pl.pallas_call(
            functools.partial(kernel, n_dev),
            out_shape=(jax.ShapeDtypeStruct((tok, width), BF16), cache_shape, cache_shape, jax.ShapeDtypeStruct((1, width), BF16)),
            in_specs=[hbm] * 10,
            out_specs=(hbm,) * 4,
            scratch_shapes=[
                pltpu.VMEM((1, width), BF16),
                pltpu.VMEM((1, width), F32),
                pltpu.VMEM((1, width), F32),
                pltpu.VMEM((1, width), F32),
                pltpu.VMEM((tok, width), BF16),
                pltpu.VMEM((1, width), BF16),
                pltpu.VMEM((rows + PAD, width), BF16),
                pltpu.VMEM((n_wo, width, wide), BF16),
                pltpu.VMEM((rows + PAD, HEAD_DIM), F32),
                pltpu.VMEM((n_chip, rows + PAD, cols), F32),
                pltpu.VMEM((2, rows + PAD, HEAD_DIM), F32),
                pltpu.VMEM((2, rows + PAD, HEAD_DIM), F32),
                pltpu.VMEM((3, n_chip, rows, cols), BF16),
                pltpu.VMEM((3, seq, cols), BF16),
                pltpu.VMEM((3, PAD, cols), BF16),
                pltpu.VMEM((heads, seq, rows), F32),
                pltpu.VMEM((heads, seq, rows), BF16),
                pltpu.VMEM((heads, HEAD_DIM, seq), BF16),
                pltpu.VMEM((n_chip, rows, cols), BF16),
                pltpu.VMEM((n_chip, tok + PAD, wide), BF16),
                pltpu.VMEM((1, cols), F32),
                pltpu.VMEM((n_dev, 1, cols), F32),
                pltpu.VMEM((tok + 8, width), F32),
                pltpu.VMEM((heads * rows, HEAD_DIM), F32),
                pltpu.VMEM((2, heads * (seq + 1), HEAD_DIM), BF16),
                dma(()), dma((4,)), dma((tok // PAD,)), dma((n_chip // 2, 2)), dma((n_wo,)), dma((2,)),
                dma(()), dma(()), dma((2,)), dma((2,)),
                dma((3, n_chip)), dma((3, n_chip)),
                dma((n_chip, 2)), dma((n_chip, 2)),
                dma((n_chip, 2)), dma((n_chip, 2)),
                dma((2,)),
            ],
            compiler_params=pltpu.CompilerParams(collective_id=0, has_side_effects=True, vmem_limit_bytes=62 * 1024 * 1024),
        )(prompt_blk[0], new_rows, w_q, w_k, w_v, w_o, q_norm_w[None], k_norm_w[None], post_norm_w[None], table)
        shape = (seq + 1, heads, HEAD_DIM)
        outs = pl.pallas_call(
            hand_over,
            out_shape=(jax.ShapeDtypeStruct((tok, width), BF16), jax.ShapeDtypeStruct(shape, BF16),
                       jax.ShapeDtypeStruct(shape, BF16), jax.ShapeDtypeStruct((1, width), BF16)),
            in_specs=[hbm] * 4,
            out_specs=(hbm,) * 4,
            scratch_shapes=[pltpu.VMEM(a.shape, BF16) for a in (outp, kc, vc, outd)] + [dma((2, 4))],
        )(outp, kc, vc, outd)
        return outs[0][None], outs[1][None], outs[2][None], outs[3]

    replicated = P()
    return jax.shard_map(
        device_step, mesh=mesh,
        in_specs=(P("dp", "sp", None), replicated, replicated, replicated, replicated, replicated, replicated, replicated, P("dp", None)),
        out_specs=(P("dp", "sp", None), P("dp", None, "sp", None), P("dp", None, "sp", None), P("dp", None)),
        check_vma=False)
```

```python
import functools
import math

import jax
import jax.numpy as jnp
import numpy as np
from jax import lax
from jax.experimental import pallas as pl
from jax.experimental.pallas import tpu as pltpu
from jax.sharding import PartitionSpec as P

HEAD_DIM = 128
ROPE_THETA = 500000.0
NORM_EPS = 1e-6
PAD = 16
VMEM_MIB = 50
LAG = 6
MASKED = -1e30
F32 = jnp.float32
BF16 = jnp.bfloat16
MESH = pl.DeviceIdType.MESH


def rope_table(seq_len):
    half = HEAD_DIM // 2
    inv_freq = np.power(np.float32(ROPE_THETA), -np.arange(0, HEAD_DIM, 2).astype(np.float32) / np.float32(HEAD_DIM)).astype(np.float32)
    pos = np.minimum(np.arange(seq_len + PAD), seq_len).astype(np.float32)
    angles = (pos[:, None] * inv_freq[None, :half]).astype(np.float32)
    return np.concatenate([np.cos(angles), np.sin(angles)], axis=-1).astype(np.float32)


def kernel(n_dev, x_hbm, new_hbm, wq, wk, wv, wo, qg_hbm, kg_hbm, pg_hbm, tab_hbm,
           outp_ref, kc_ref, vc_ref, outd_ref,
           new_ref, qg_ref, kg_ref, pg_ref,
           xs, pool, tab, raw, ssq, ssq_in, send, recv, new, s_ref, p_ref, vt, osend, orecv, dsend, dsum, acc, stage,
           xsem, insem, wsem, wosem, tabsem, xs_s, xs_r, ss_s, ss_r, a_s, a_r, d_s, d_r, o_s, o_r):
    tok = x_hbm.shape[0]
    width = x_hbm.shape[1]
    rows = 2 * tok
    n_chip = n_dev // 2
    half_chip = n_chip // 2
    cols = width // n_dev
    heads = cols // HEAD_DIM
    seq = tok * n_dev
    n_step = n_chip // 2
    n_wo = pool.shape[0]
    wide = 2 * cols

    me = lax.axis_index("sp")
    chip = lax.div(me, 2)
    core = lax.rem(me, 2)
    sibling = 2 * chip + (1 - core)

    def offset_of(idx):
        odd = lax.rem(idx, 2)
        return lax.rem(half_chip + odd + (2 * odd - 1) * lax.div(idx, 2), n_chip)

    def group_col(idx):
        dest = lax.rem(chip + offset_of(idx), n_chip)
        return pl.multiple_of((2 * dest + core) * cols, cols)

    def w_copy(w_ref, s, half):
        return pltpu.make_async_copy(
            w_ref.at[:, pl.ds(group_col(2 * s + half), cols)], pool.at[s, :, pl.ds(half * cols, cols)], wsem.at[s, half])

    def wo_copy(j):
        return pltpu.make_async_copy(wo.at[:, pl.ds(pl.multiple_of(j * wide, wide), wide)], pool.at[j], wosem.at[j])

    my_rows = pl.ds(pl.multiple_of(core * tok, tok), tok)
    x_copy = pltpu.make_async_copy(x_hbm, xs.at[my_rows], xsem)
    x_copy.start()
    smalls = [pltpu.make_async_copy(a, b, insem.at[n]) for n, (a, b) in enumerate(
        ((new_hbm, new_ref), (qg_hbm, qg_ref), (kg_hbm, kg_ref), (pg_hbm, pg_ref)))]
    w_copy(wv, 0, 0).start()
    w_copy(wv, 0, 1).start()
    for small in smalls:
        small.start()
    tab_a = pltpu.make_async_copy(tab_hbm.at[pl.ds(pl.multiple_of(chip * rows, rows), rows)], tab.at[pl.ds(0, rows)], tabsem.at[0])
    tab_b = pltpu.make_async_copy(tab_hbm.at[pl.ds(seq, PAD)], tab.at[pl.ds(rows, PAD)], tabsem.at[1])
    tab_a.start()
    tab_b.start()

    barrier = pltpu.get_barrier_semaphore()
    for off in range(1, n_dev):
        pl.semaphore_signal(barrier, inc=1, device_id={"sp": lax.rem(me + off, n_dev)}, device_id_type=MESH)
    x_copy.wait()
    for s in range(1, n_step):
        w_copy(wv, s, 0).start()
        w_copy(wv, s, 1).start()

    own_rows = pl.ds(pl.multiple_of(chip * rows, rows), rows)

    def exchange(t, idx):
        dest = lax.rem(chip + offset_of(idx), n_chip)
        return pltpu.make_async_remote_copy(
            src_ref=send.at[t, idx], dst_ref=recv.at[t, own_rows], send_sem=a_s.at[t, idx], recv_sem=a_r.at[t, idx],
            device_id={"sp": 2 * dest + core}, device_id_type=MESH)

    def emit(t, idx, block):
        @pl.when(idx < n_chip - 1)
        def _():
            send[t, idx] = block[:rows]
            exchange(t, idx).start()

        @pl.when(idx == n_chip - 1)
        def _():
            recv[t, own_rows, :] = block[:rows]
            new[t] = block[rows:]

    def project(s):
        w_copy(wv, s, 0).wait()
        w_copy(wv, s, 1).wait()
        return jnp.dot(xs[...], pool[s], preferred_element_type=F32)

    def half_exchange(idx, which, row):
        dest = lax.rem(chip + offset_of(idx), n_chip)
        at = pl.ds(pl.multiple_of(which * tok, tok), tok)
        return pltpu.make_async_remote_copy(
            src_ref=send.at[2, idx, at], dst_ref=recv.at[2, pl.ds(pl.multiple_of(chip * rows + which * tok, tok), tok)],
            send_sem=a_s.at[row, idx], recv_sem=a_r.at[row, idx], device_id={"sp": 2 * dest + core}, device_id_type=MESH)

    def half_project(which):
        at = pl.ds(pl.multiple_of(which * tok, tok), tok)
        res = jnp.dot(xs[at, :], pool[0], preferred_element_type=F32).astype(BF16)
        for idx in range(2):
            send[2, idx, at, :] = res[:, idx * cols:(idx + 1) * cols]

    w_copy(wv, 0, 0).wait()
    w_copy(wv, 0, 1).wait()
    with jax.named_scope("v_first"):
        half_project(core)
    with jax.named_scope("barrier"):
        pl.semaphore_wait(barrier, n_dev - 1)
    x_send = pltpu.make_async_remote_copy(
        src_ref=xs.at[my_rows], dst_ref=xs.at[my_rows], send_sem=xs_s, recv_sem=xs_r, device_id={"sp": sibling}, device_id_type=MESH)
    x_send.start()
    for idx in range(2):
        half_exchange(idx, core, 3).start()
    for small in smalls:
        small.wait()
    xs[pl.ds(rows, PAD), :] = jnp.broadcast_to(new_ref[...], (PAD, width))
    acc[...] = jnp.zeros_like(acc)
    with jax.named_scope("x_arrive"):
        x_send.wait_recv()

    def v_step(s, carry):
        res = project(s)
        w_copy(wk, s, 0).start()
        w_copy(wk, s, 1).start()
        for half in range(2):
            emit(2, 2 * s + half, res[:, half * cols:(half + 1) * cols].astype(BF16))
        return carry

    with jax.named_scope('v_proj'):
        lax.fori_loop(1, n_step, v_step, 0)
        half_project(1 - core)
        for idx in range(2):
            half_exchange(idx, 1 - core, 2).start()
        w_copy(wk, 0, 0).start()
        w_copy(wk, 0, 1).start()
    tab_a.wait()
    tab_b.wait()

    lane = lax.broadcasted_iota(jnp.int32, (rows + PAD, HEAD_DIM), 1)
    first = lane < HEAD_DIM // 2

    def raw_step(t, i):
        s = lax.rem(i + 1, n_step)
        res = project(s)
        sq = jnp.zeros((rows + PAD, HEAD_DIM), F32)
        for half in range(2):
            part = res[:, half * cols:(half + 1) * cols]
            raw[2 * s + half] = part
            for h in range(heads):
                piece = part[:, h * HEAD_DIM:(h + 1) * HEAD_DIM]
                sq = sq + piece * piece
        @pl.when(i == 0)
        def _():
            ssq[t] = sq

        @pl.when(i > 0)
        def _():
            ssq[t] += sq

        return s

    def norm_and_send(t, g_ref):
        swap = pltpu.make_async_remote_copy(
            src_ref=ssq.at[t], dst_ref=ssq_in.at[t], send_sem=ss_s.at[t], recv_sem=ss_r.at[t],
            device_id={"sp": sibling}, device_id_type=MESH)
        swap.start()
        swap.wait_recv()
        total = jnp.sum(ssq[t] + ssq_in[t], axis=1, keepdims=True)
        scale = lax.rsqrt(total * (1.0 / width) + NORM_EPS)

        def one(idx, carry):
            g = g_ref[:, pl.ds(group_col(idx), cols)]
            table = tab[...]
            turned = pltpu.roll(table, HEAD_DIM // 2, 1)
            cos = jnp.where(first, table, turned)
            sin = jnp.where(first, -turned, table)
            parts = []
            for h in range(heads):
                at = slice(h * HEAD_DIM, (h + 1) * HEAD_DIM)
                val = raw[idx, :, at] * scale * g[:, at]
                parts.append((val * cos + pltpu.roll(val, HEAD_DIM // 2, 1) * sin).astype(BF16))
            emit(t, idx, jnp.concatenate(parts, axis=1))
            return carry

        lax.fori_loop(0, n_chip, one, 0)

    def k_step(i, carry):
        s = raw_step(1, i)
        w_copy(wq, s, 0).start()
        w_copy(wq, s, 1).start()
        return carry

    with jax.named_scope('k_proj'):
        lax.fori_loop(0, n_step, k_step, 0)
    with jax.named_scope('k_norm'):
        norm_and_send(1, kg_ref)
    for j in range(n_step, n_wo):
        wo_copy(j).start()

    def q_step(i, carry):
        s = raw_step(0, i)
        wo_copy(s).start()
        return carry

    with jax.named_scope('q_proj'):
        lax.fori_loop(0, n_step, q_step, 0)
    with jax.named_scope('q_norm'):
        norm_and_send(0, qg_ref)

    def arrivals(t, start=0):
        def one(idx, carry):
            exchange(t, idx).wait_recv()
            return carry
        lax.fori_loop(start, n_chip - 1, one, 0)

    def fill_cache(t, cache):
        def one(b, carry):
            base = pl.multiple_of(b * rows, rows)
            block = recv[t, pl.ds(base, rows), :].astype(F32)
            for h in range(heads):
                stage[pl.ds(h, rows, stride=heads), :] = block[:, h * HEAD_DIM:(h + 1) * HEAD_DIM]
            cache[pl.ds(pl.multiple_of(heads * base, heads * rows), heads * rows), :] = stage[...].astype(BF16)
            return carry
        lax.fori_loop(0, n_chip, one, 0)
        last = new[t][0:1, :].astype(F32)
        rows_new = jnp.concatenate([last[:, h * HEAD_DIM:(h + 1) * HEAD_DIM] for h in range(heads)], axis=0)
        cache[pl.ds(heads * seq, heads), :] = rows_new.astype(BF16)

    with jax.named_scope("v_arrive"):
        for idx in range(2):
            half_exchange(idx, core, 3).wait_recv()
            half_exchange(idx, 1 - core, 2).wait_recv()
        arrivals(2, 2)
    with jax.named_scope("v_cache"):
        fill_cache(2, vc_ref)
        for b in range(n_chip):
            for h in range(heads):
                vt[h, :, b * rows:(b + 1) * rows] = recv[2, b * rows:(b + 1) * rows, h * HEAD_DIM:(h + 1) * HEAD_DIM].astype(F32).T.astype(BF16)
    with jax.named_scope("k_arrive"):
        arrivals(1)
    with jax.named_scope("k_cache"):
        fill_cache(1, kc_ref)

    log_scale = HEAD_DIM ** -0.5 * math.log2(math.e)
    contract_last = (((1,), (1,)), ((), ()))

    for h in range(heads):
        at = slice(h * HEAD_DIM, (h + 1) * HEAD_DIM)
        qd, kd, vd = new[0][:, at], new[1][:, at], new[2][:, at]
        sc = lax.dot_general(qd, recv[1, :, at], contract_last, preferred_element_type=F32) * log_scale
        sn = jnp.sum(qd.astype(F32) * kd.astype(F32), axis=1, keepdims=True) * log_scale
        top = jnp.maximum(jnp.max(sc, axis=1, keepdims=True), sn)
        ex = jnp.exp2(sc - top)
        en = jnp.exp2(sn - top)
        inv = 1.0 / (jnp.sum(ex, axis=1, keepdims=True) + en)
        prob = (ex * inv).astype(BF16)
        prob_n = (en * inv).astype(BF16).astype(F32)
        od = jnp.dot(prob, recv[2, :, at], preferred_element_type=F32) + prob_n * vd.astype(F32)
        dsend[:, at] = od[0:1].astype(BF16).astype(F32)

    def d_copy(off, kk, to):
        return pltpu.make_async_remote_copy(
            src_ref=dsend, dst_ref=dsum.at[2 * off + core], send_sem=d_s.at[off, kk], recv_sem=d_r.at[off, core],
            device_id={"sp": to}, device_id_type=MESH)

    d_copy(0, 0, sibling).start()
    for off in range(1, n_chip):
        for kk in range(2):
            d_copy(off, kk, 2 * lax.rem(chip + off, n_chip) + kk).start()
    dsum[core] = dsend[...]

    def o_copy(i, kk, to, off_o):
        return pltpu.make_async_remote_copy(
            src_ref=osend.at[i, pl.ds(pl.multiple_of(kk * tok, tok), tok)],
            dst_ref=orecv.at[off_o, pl.ds(0, tok), pl.ds(pl.multiple_of(core * cols, cols), cols)],
            send_sem=o_s.at[i, kk], recv_sem=o_r.at[off_o, core], device_id={"sp": to}, device_id_type=MESH)

    def fold(block, op):
        return op(block.reshape(block.shape[0] // 8, 8, block.shape[1]), axis=0)

    def attend(i):
        idx = lax.rem(i + n_chip - 1, n_chip)
        off_q = offset_of(idx)
        src = lax.rem(chip + n_chip - off_q, n_chip)
        off_o = lax.rem(n_chip - off_q, n_chip)

        @pl.when(i > 0)
        def _():
            with jax.named_scope("q_arrive"):
                exchange(0, idx).wait_recv()

        src_at = pl.ds(pl.multiple_of(src * rows, rows), rows)
        causal = lax.broadcasted_iota(jnp.int32, (rows, rows), 0) <= lax.broadcasted_iota(jnp.int32, (rows, rows), 1)
        blocks = [slice(kb * rows, (kb + 1) * rows) for kb in range(n_chip)]
        tops = []
        for h in range(heads):
            at = slice(h * HEAD_DIM, (h + 1) * HEAD_DIM)
            sc = lax.dot_general(recv[1, :, at], recv[0, src_at, at], contract_last, preferred_element_type=F32)
            s_ref[h] = sc
            top = jnp.full((8, rows), -jnp.inf, F32)
            for kb in range(n_chip):
                top = jnp.maximum(top, fold(sc[blocks[kb]], jnp.max) + jnp.where(kb < src, 0.0, -jnp.inf))
            tops.append(top)
        for h in range(heads):
            at = slice(h * HEAD_DIM, (h + 1) * HEAD_DIM)
            own = jnp.where(causal, s_ref[h, src_at, :], -jnp.inf)
            s_ref[h, src_at, :] = own
            top = jnp.max(jnp.maximum(tops[h], fold(own, jnp.max)), axis=0, keepdims=True) * log_scale
            total = jnp.zeros((8, rows), F32)
            for kb in range(n_chip):
                ex = jnp.exp2(s_ref[h, blocks[kb], :] * log_scale + (jnp.where(kb <= src, 0.0, -jnp.inf) - top))
                s_ref[h, blocks[kb], :] = ex
                total = total + fold(ex, jnp.sum)
            inv = 1.0 / jnp.sum(total, axis=0, keepdims=True)
            for kb in range(n_chip):
                p_ref[h, blocks[kb], :] = (s_ref[h, blocks[kb], :] * inv).astype(BF16)
            osend[i, :, at] = jnp.dot(vt[h], p_ref[h], preferred_element_type=F32).T.astype(BF16)

        @pl.when(i > 0)
        def _():
            for kk in range(2):
                o_copy(i, kk, 2 * src + kk, off_o).start()

        @pl.when(i == 0)
        def _():
            o_copy(i, 1 - core, sibling, off_o).start()
            orecv[0, pl.ds(0, tok), pl.ds(pl.multiple_of(core * cols, cols), cols)] = osend[0, my_rows, :]

    zero_half = jnp.zeros((8, cols), BF16)

    def gather(i):
        off_o = lax.rem(n_chip - offset_of(lax.rem(i + n_chip - 1, n_chip)), n_chip)
        src = lax.rem(chip + n_chip - off_o, n_chip)

        def wait_pair(kk):
            pltpu.make_async_remote_copy(
                src_ref=osend.at[0, pl.ds(0, tok)], dst_ref=orecv.at[off_o, pl.ds(0, tok), pl.ds(pl.multiple_of(kk * cols, cols), cols)],
                send_sem=o_s.at[0, 0], recv_sem=o_r.at[off_o, kk], device_id={"sp": sibling}, device_id_type=MESH).wait_recv()
            pltpu.make_async_remote_copy(
                src_ref=dsend, dst_ref=dsum.at[2 * off_o + kk], send_sem=d_s.at[0, 0], recv_sem=d_r.at[off_o, kk],
                device_id={"sp": sibling}, device_id_type=MESH).wait_recv()

        @pl.when(i == 0)
        def _():
            wait_pair(1 - core)

        @pl.when(i > 0)
        def _():
            with jax.named_scope("o_arrive"):
                wait_pair(0)
                wait_pair(1)

        d0 = jnp.broadcast_to(dsum[2 * off_o].astype(BF16), (8, cols))
        d1 = jnp.broadcast_to(dsum[2 * off_o + 1].astype(BF16), (8, cols))
        orecv[off_o, pl.ds(tok, PAD), :] = jnp.concatenate(
            [jnp.concatenate([d0, zero_half], axis=1), jnp.concatenate([zero_half, d1], axis=1)], axis=0)
        k_at = pl.ds(pl.multiple_of(src * wide, wide), wide)
        lhs = orecv[off_o]
        for j in range(n_wo):
            res = jnp.dot(lhs, pool[j, k_at, :], preferred_element_type=F32)
            parts = res[tok:tok + 8].astype(BF16).astype(F32) + res[tok + 8:].astype(BF16).astype(F32)
            n_at = slice(j * wide, (j + 1) * wide)
            acc[pl.ds(0, tok), n_at] += res[:tok]
            acc[pl.ds(tok, 8), n_at] += parts

    def drain_early():
        x_send.wait_send()
        for t in range(2):
            pltpu.make_async_remote_copy(
                src_ref=ssq.at[t], dst_ref=ssq_in.at[t], send_sem=ss_s.at[t], recv_sem=ss_r.at[t],
                device_id={"sp": sibling}, device_id_type=MESH).wait_send()

        def drain(idx, carry):
            for t in range(2):
                exchange(t, idx).wait_send()

            @pl.when(idx >= 2)
            def _():
                exchange(2, idx).wait_send()

            for kk in range(2):
                d_copy(idx + 1, kk, sibling).wait_send()
            return carry

        lax.fori_loop(0, n_chip - 1, drain, 0)
        for idx in range(2):
            half_exchange(idx, core, 3).wait_send()
            half_exchange(idx, 1 - core, 2).wait_send()
        d_copy(0, 0, sibling).wait_send()

    def both(i, carry):
        @pl.when(i < n_chip)
        def _():
            with jax.named_scope("attend"):
                attend(i)

        @pl.when(i == LAG)
        def _():
            for j in range(n_wo):
                wo_copy(j).wait()
            drain_early()

        @pl.when(i >= LAG)
        def _():
            with jax.named_scope("gather"):
                gather(i - LAG)
        return carry

    lax.fori_loop(0, n_chip + LAG, both, 0)

    def finish(r, carry):
        r_at = pl.ds(pl.multiple_of(r * PAD, PAD), PAD)
        val = acc[r_at, :]
        scale = lax.rsqrt(jnp.sum(val * val, axis=1, keepdims=True) * (1.0 / width) + NORM_EPS)
        x_at = pl.ds(pl.multiple_of(core * tok + r * PAD, PAD), PAD)
        outp_ref[r_at, :] = (xs[x_at, :].astype(F32) + val * scale * pg_ref[...]).astype(BF16)
        return carry

    with jax.named_scope("finish"):
        lax.fori_loop(0, tok // PAD, finish, 0)
        val = acc[pl.ds(tok, 8), :]
        scale = lax.rsqrt(jnp.sum(val * val, axis=1, keepdims=True) * (1.0 / width) + NORM_EPS)
        outd_ref[...] = (new_ref[...].astype(F32) + (val * scale * pg_ref[...])[0:1]).astype(BF16)

    def drain_o(idx, carry):
        for kk in range(2):
            o_copy(idx + 1, kk, sibling, 0).wait_send()
        return carry

    lax.fori_loop(0, n_chip - 1, drain_o, 0)
    o_copy(0, 1 - core, sibling, 0).wait_send()


def hand_over(outp_in, kc_in, vc_in, outd_in, outp, kc, vc, outd, sem):
    outs = [pltpu.make_async_copy(a, b, sem.at[n]) for n, (a, b) in enumerate(
        ((outp_in, outp), (kc_in, kc.reshape(kc_in.shape)), (vc_in, vc.reshape(vc_in.shape)), (outd_in, outd)))]
    for one in outs:
        one.start()
    for one in outs:
        one.wait()


def solution(mesh):
    n_dev = mesh.shape["sp"]

    def device_step(prompt_blk, w_q, w_k, w_v, w_o, q_norm_w, k_norm_w, post_norm_w, new_rows):
        _, tok, width = prompt_blk.shape
        n_chip = n_dev // 2
        rows, seq, cols = 2 * tok, tok * n_dev, width // n_dev
        heads = cols // HEAD_DIM
        wide = 2 * cols
        n_wo = width // wide
        table = jnp.asarray(rope_table(seq))
        hbm = pl.BlockSpec(memory_space=pltpu.HBM)
        vmem = pl.BlockSpec(memory_space=pltpu.VMEM)
        dma = pltpu.SemaphoreType.DMA
        cache_shape = jax.ShapeDtypeStruct((heads * (seq + 1), HEAD_DIM), BF16)

        def keep(value):
            return pltpu.with_memory_space_constraint(value, pltpu.HBM)

        outp, kc, vc, outd = pl.pallas_call(
            functools.partial(kernel, n_dev),
            out_shape=(jax.ShapeDtypeStruct((tok, width), BF16), cache_shape, cache_shape, jax.ShapeDtypeStruct((1, width), BF16)),
            in_specs=[hbm] * 10,
            out_specs=(vmem,) * 4,
            scratch_shapes=[
                pltpu.VMEM((1, width), BF16),
                pltpu.VMEM((1, width), F32),
                pltpu.VMEM((1, width), F32),
                pltpu.VMEM((1, width), F32),
                pltpu.VMEM((rows + PAD, width), BF16),
                pltpu.VMEM((n_wo, width, wide), BF16),
                pltpu.VMEM((rows + PAD, HEAD_DIM), F32),
                pltpu.VMEM((n_chip, rows + PAD, cols), F32),
                pltpu.VMEM((2, rows + PAD, HEAD_DIM), F32),
                pltpu.VMEM((2, rows + PAD, HEAD_DIM), F32),
                pltpu.VMEM((3, n_chip, rows, cols), BF16),
                pltpu.VMEM((3, seq, cols), BF16),
                pltpu.VMEM((3, PAD, cols), BF16),
                pltpu.VMEM((heads, seq, rows), F32),
                pltpu.VMEM((heads, seq, rows), BF16),
                pltpu.VMEM((heads, HEAD_DIM, seq), BF16),
                pltpu.VMEM((n_chip, rows, cols), BF16),
                pltpu.VMEM((n_chip, tok + PAD, wide), BF16),
                pltpu.VMEM((1, cols), F32),
                pltpu.VMEM((n_dev, 1, cols), F32),
                pltpu.VMEM((tok + 8, width), F32),
                pltpu.VMEM((heads * rows, HEAD_DIM), F32),
                dma(()), dma((4,)), dma((n_chip // 2, 2)), dma((n_wo,)), dma((2,)),
                dma(()), dma(()), dma((2,)), dma((2,)),
                dma((4, n_chip)), dma((4, n_chip)),
                dma((n_chip, 2)), dma((n_chip, 2)),
                dma((n_chip, 2)), dma((n_chip, 2)),
            ],
            compiler_params=pltpu.CompilerParams(collective_id=0, has_side_effects=True, vmem_limit_bytes=VMEM_MIB * 1024 * 1024),
        )(keep(prompt_blk[0]), keep(new_rows), w_q, w_k, w_v, w_o, keep(q_norm_w[None]), keep(k_norm_w[None]), keep(post_norm_w[None]), keep(table))
        shape = (seq + 1, heads, HEAD_DIM)
        outs = pl.pallas_call(
            hand_over,
            out_shape=(jax.ShapeDtypeStruct((tok, width), BF16), jax.ShapeDtypeStruct(shape, BF16),
                       jax.ShapeDtypeStruct(shape, BF16), jax.ShapeDtypeStruct((1, width), BF16)),
            in_specs=[vmem] * 4,
            out_specs=(hbm,) * 4,
            scratch_shapes=[dma((4,))],
            compiler_params=pltpu.CompilerParams(vmem_limit_bytes=8 * 1024 * 1024),
        )(outp, kc, vc, outd)
        return outs[0][None], outs[1][None], outs[2][None], outs[3]

    replicated = P()
    return jax.shard_map(
        device_step, mesh=mesh,
        in_specs=(P("dp", "sp", None), replicated, replicated, replicated, replicated, replicated, replicated, replicated, P("dp", None)),
        out_specs=(P("dp", "sp", None), P("dp", None, "sp", None), P("dp", None, "sp", None), P("dp", None)),
        check_vma=False)
```

```python
import functools
import math

import jax
import jax.numpy as jnp
import numpy as np
from jax import lax
from jax.experimental import pallas as pl
from jax.experimental.pallas import tpu as pltpu
from jax.sharding import PartitionSpec as P

HEAD_DIM = 128
ROPE_THETA = 500000.0
NORM_EPS = 1e-6
PAD = 16
VMEM_MIB = 50
LAG = 6
MASKED = -1e30
F32 = jnp.float32
BF16 = jnp.bfloat16
MESH = pl.DeviceIdType.MESH


def rope_table(seq_len):
    half = HEAD_DIM // 2
    inv_freq = np.power(np.float32(ROPE_THETA), -np.arange(0, HEAD_DIM, 2).astype(np.float32) / np.float32(HEAD_DIM)).astype(np.float32)
    pos = np.minimum(np.arange(seq_len + PAD), seq_len).astype(np.float32)
    angles = (pos[:, None] * inv_freq[None, :half]).astype(np.float32)
    return np.concatenate([np.cos(angles), np.sin(angles)], axis=-1).astype(np.float32)


def kernel(n_dev, x_hbm, new_hbm, wq, wk, wv, wo, qg_hbm, kg_hbm, pg_hbm, tab_hbm,
           outp_ref, kc_ref, vc_ref, outd_ref,
           new_ref, gains,
           xs, pool, tab, raw, ssq, ssq_in, send, recv, new, s_ref, p_ref, vt, osend, orecv, dsend, dsum, acc, stage,
           xsem, insem, wsem, wosem, tabsem, xs_s, xs_r, ss_s, ss_r, a_s, a_r, q_r, d_s, d_r, o_s, o_r):
    tok = x_hbm.shape[0]
    width = x_hbm.shape[1]
    rows = 2 * tok
    n_chip = n_dev // 2
    half_chip = n_chip // 2
    cols = width // n_dev
    heads = cols // HEAD_DIM
    seq = tok * n_dev
    n_step = n_chip // 2
    n_wo = pool.shape[0]
    wide = 2 * cols

    me = lax.axis_index("sp")
    chip = lax.div(me, 2)
    core = lax.rem(me, 2)
    sibling = 2 * chip + (1 - core)

    def offset_of(idx):
        odd = lax.rem(idx, 2)
        return lax.rem(half_chip + odd + (2 * odd - 1) * lax.div(idx, 2), n_chip)

    def group_col(idx):
        dest = lax.rem(chip + offset_of(idx), n_chip)
        return pl.multiple_of((2 * dest + core) * cols, cols)

    def w_copy(w_ref, s, half):
        return pltpu.make_async_copy(
            w_ref.at[:, pl.ds(group_col(2 * s + half), cols)], pool.at[s, :, pl.ds(half * cols, cols)], wsem.at[s])

    def w_wait(s):
        pltpu.make_async_copy(pool.at[s], pool.at[s], wsem.at[s]).wait()

    def wo_copy(j):
        return pltpu.make_async_copy(wo.at[:, pl.ds(pl.multiple_of(j * wide, wide), wide)], pool.at[j], wosem)

    barrier = pltpu.get_barrier_semaphore()
    for off in sorted(range(1, n_dev), key=lambda off: -min(off, n_dev - off)):
        pl.semaphore_signal(barrier, inc=1, device_id={"sp": lax.rem(me + off, n_dev)}, device_id_type=MESH)

    my_rows = pl.ds(pl.multiple_of(core * tok, tok), tok)
    x_copy = pltpu.make_async_copy(x_hbm, xs.at[my_rows], xsem)
    x_copy.start()
    smalls = [pltpu.make_async_copy(a, b, insem.at[n]) for a, b, n in (
        (new_hbm, new_ref, 0), (qg_hbm, gains.at[0], 1), (kg_hbm, gains.at[1], 1), (pg_hbm, gains.at[2], 1))]
    w_copy(wv, 0, 0).start()
    w_copy(wv, 0, 1).start()
    for small in smalls:
        small.start()
    tab_a = pltpu.make_async_copy(tab_hbm.at[pl.ds(pl.multiple_of(chip * rows, rows), rows)], tab.at[pl.ds(0, rows)], tabsem)
    tab_b = pltpu.make_async_copy(tab_hbm.at[pl.ds(seq, PAD)], tab.at[pl.ds(rows, PAD)], tabsem)
    tab_a.start()
    tab_b.start()

    x_copy.wait()
    for s in range(1, n_step):
        w_copy(wv, s, 0).start()
        w_copy(wv, s, 1).start()

    own_rows = pl.ds(pl.multiple_of(chip * rows, rows), rows)

    def exchange(t, idx):
        dest = lax.rem(chip + offset_of(idx), n_chip)
        return pltpu.make_async_remote_copy(
            src_ref=send.at[t, idx], dst_ref=recv.at[t, own_rows], send_sem=a_s.at[t], recv_sem=a_r.at[t] if t else q_r.at[idx],
            device_id={"sp": 2 * dest + core}, device_id_type=MESH)

    def emit(t, idx, block):
        @pl.when(idx < n_chip - 1)
        def _():
            send[t, idx] = block[:rows]
            exchange(t, idx).start()

        @pl.when(idx == n_chip - 1)
        def _():
            recv[t, own_rows, :] = block[:rows]
            new[t] = block[rows:]

    def project(s):
        w_wait(s)
        return jnp.dot(xs[...], pool[s], preferred_element_type=F32)

    def half_exchange(idx, which):
        dest = lax.rem(chip + offset_of(idx), n_chip)
        at = pl.ds(pl.multiple_of(which * tok, tok), tok)
        return pltpu.make_async_remote_copy(
            src_ref=send.at[2, idx, at], dst_ref=recv.at[2, pl.ds(pl.multiple_of(chip * rows + which * tok, tok), tok)],
            send_sem=a_s.at[2], recv_sem=a_r.at[2], device_id={"sp": 2 * dest + core}, device_id_type=MESH)

    def half_project(which):
        at = pl.ds(pl.multiple_of(which * tok, tok), tok)
        res = jnp.dot(xs[at, :], pool[0], preferred_element_type=F32).astype(BF16)
        for idx in range(2):
            send[2, idx, at, :] = res[:, idx * cols:(idx + 1) * cols]

    w_wait(0)
    with jax.named_scope("v_first"):
        half_project(core)
    with jax.named_scope("barrier"):
        pl.semaphore_wait(barrier, n_dev - 1)
    x_send = pltpu.make_async_remote_copy(
        src_ref=xs.at[my_rows], dst_ref=xs.at[my_rows], send_sem=xs_s, recv_sem=xs_r, device_id={"sp": sibling}, device_id_type=MESH)
    x_send.start()
    for idx in range(2):
        half_exchange(idx, core).start()
    smalls[0].wait()
    pltpu.make_async_copy(gains, gains, insem.at[1]).wait()
    xs[pl.ds(rows, PAD), :] = jnp.broadcast_to(new_ref[...], (PAD, width))
    acc[...] = jnp.zeros_like(acc)
    with jax.named_scope("x_arrive"):
        x_send.wait_recv()

    def v_step(s, carry):
        res = project(s)
        w_copy(wk, s, 0).start()
        w_copy(wk, s, 1).start()
        for half in range(2):
            emit(2, 2 * s + half, res[:, half * cols:(half + 1) * cols].astype(BF16))
        return carry

    with jax.named_scope('v_proj'):
        lax.fori_loop(1, n_step, v_step, 0)
        half_project(1 - core)
        for idx in range(2):
            half_exchange(idx, 1 - core).start()
        w_copy(wk, 0, 0).start()
        w_copy(wk, 0, 1).start()
    pltpu.make_async_copy(tab, tab, tabsem).wait()

    lane = lax.broadcasted_iota(jnp.int32, (rows + PAD, HEAD_DIM), 1)
    first = lane < HEAD_DIM // 2

    def raw_step(t, i):
        s = lax.rem(i + 1, n_step)
        res = project(s)
        sq = jnp.zeros((rows + PAD, HEAD_DIM), F32)
        for half in range(2):
            part = res[:, half * cols:(half + 1) * cols]
            raw[2 * s + half] = part
            for h in range(heads):
                piece = part[:, h * HEAD_DIM:(h + 1) * HEAD_DIM]
                sq = sq + piece * piece
        @pl.when(i == 0)
        def _():
            ssq[t] = sq

        @pl.when(i > 0)
        def _():
            ssq[t] += sq

        return s

    def norm_and_send(t, g_ref):
        swap = pltpu.make_async_remote_copy(
            src_ref=ssq.at[t], dst_ref=ssq_in.at[t], send_sem=ss_s.at[t], recv_sem=ss_r.at[t],
            device_id={"sp": sibling}, device_id_type=MESH)
        swap.start()
        swap.wait_recv()
        total = jnp.sum(ssq[t] + ssq_in[t], axis=1, keepdims=True)
        scale = lax.rsqrt(total * (1.0 / width) + NORM_EPS)

        def one(n, carry):
            idx = n if t else n_chip - 1 - n
            g = g_ref[:, pl.ds(group_col(idx), cols)]
            table = tab[...]
            turned = pltpu.roll(table, HEAD_DIM // 2, 1)
            cos = jnp.where(first, table, turned)
            sin = jnp.where(first, -turned, table)
            parts = []
            for h in range(heads):
                at = slice(h * HEAD_DIM, (h + 1) * HEAD_DIM)
                val = raw[idx, :, at] * scale * g[:, at]
                parts.append((val * cos + pltpu.roll(val, HEAD_DIM // 2, 1) * sin).astype(BF16))
            emit(t, idx, jnp.concatenate(parts, axis=1))
            return carry

        lax.fori_loop(0, n_chip, one, 0)

    def k_step(i, carry):
        s = raw_step(1, i)
        w_copy(wq, s, 0).start()
        w_copy(wq, s, 1).start()
        return carry

    with jax.named_scope('k_proj'):
        lax.fori_loop(0, n_step, k_step, 0)
    with jax.named_scope('k_norm'):
        norm_and_send(1, gains.at[1])
    for j in range(n_step, n_wo):
        wo_copy(j).start()

    def q_step(i, carry):
        s = raw_step(0, i)
        wo_copy(s).start()
        return carry

    with jax.named_scope('q_proj'):
        lax.fori_loop(0, n_step, q_step, 0)
    with jax.named_scope('q_norm'):
        norm_and_send(0, gains.at[0])

    def whole(t):
        every = pl.ds(0, (n_chip - 1) * rows)
        return pltpu.make_async_remote_copy(
            src_ref=recv.at[t, every], dst_ref=recv.at[t, every], send_sem=a_s.at[t], recv_sem=a_r.at[t],
            device_id={"sp": sibling}, device_id_type=MESH)

    def fill_cache(t, cache):
        def one(b, carry):
            base = pl.multiple_of(b * rows, rows)
            block = recv[t, pl.ds(base, rows), :].astype(F32)
            for h in range(heads):
                stage[pl.ds(h, rows, stride=heads), :] = block[:, h * HEAD_DIM:(h + 1) * HEAD_DIM]
            cache[pl.ds(pl.multiple_of(heads * base, heads * rows), heads * rows), :] = stage[...].astype(BF16)
            return carry
        lax.fori_loop(0, n_chip, one, 0)
        last = new[t][0:1, :].astype(F32)
        rows_new = jnp.concatenate([last[:, h * HEAD_DIM:(h + 1) * HEAD_DIM] for h in range(heads)], axis=0)
        cache[pl.ds(heads * seq, heads), :] = rows_new.astype(BF16)

    with jax.named_scope("v_arrive"):
        whole(2).wait_recv()
    with jax.named_scope("v_cache"):
        fill_cache(2, vc_ref)
        for b in range(n_chip):
            for h in range(heads):
                vt[h, :, b * rows:(b + 1) * rows] = recv[2, b * rows:(b + 1) * rows, h * HEAD_DIM:(h + 1) * HEAD_DIM].astype(F32).T.astype(BF16)
    with jax.named_scope("k_arrive"):
        whole(1).wait_recv()
    with jax.named_scope("k_cache"):
        fill_cache(1, kc_ref)

    log_scale = HEAD_DIM ** -0.5 * math.log2(math.e)
    contract_last = (((1,), (1,)), ((), ()))

    for h in range(heads):
        at = slice(h * HEAD_DIM, (h + 1) * HEAD_DIM)
        qd, kd, vd = new[0][:, at], new[1][:, at], new[2][:, at]
        sc = lax.dot_general(qd, recv[1, :, at], contract_last, preferred_element_type=F32) * log_scale
        sn = jnp.sum(qd.astype(F32) * kd.astype(F32), axis=1, keepdims=True) * log_scale
        top = jnp.maximum(jnp.max(sc, axis=1, keepdims=True), sn)
        ex = jnp.exp2(sc - top)
        en = jnp.exp2(sn - top)
        inv = 1.0 / (jnp.sum(ex, axis=1, keepdims=True) + en)
        prob = (ex * inv).astype(BF16)
        prob_n = (en * inv).astype(BF16).astype(F32)
        od = jnp.dot(prob, recv[2, :, at], preferred_element_type=F32) + prob_n * vd.astype(F32)
        dsend[:, at] = od[0:1].astype(BF16).astype(F32)

    def d_copy(off, to):
        return pltpu.make_async_remote_copy(
            src_ref=dsend, dst_ref=dsum.at[2 * off + core], send_sem=d_s, recv_sem=d_r,
            device_id={"sp": to}, device_id_type=MESH)

    d_copy(0, sibling).start()
    for off in range(1, n_chip):
        for kk in range(2):
            d_copy(off, 2 * lax.rem(chip + off, n_chip) + kk).start()
    dsum[core] = dsend[...]

    def d_whole():
        every = pl.ds(0, n_dev - 1)
        return pltpu.make_async_remote_copy(
            src_ref=dsum.at[every], dst_ref=dsum.at[every], send_sem=d_s, recv_sem=d_r,
            device_id={"sp": sibling}, device_id_type=MESH)

    def o_copy(i, kk, to, off_o, near=0):
        return pltpu.make_async_remote_copy(
            src_ref=osend.at[i, pl.ds(pl.multiple_of(kk * tok, tok), tok)],
            dst_ref=orecv.at[off_o, pl.ds(0, tok), pl.ds(pl.multiple_of(core * cols, cols), cols)],
            send_sem=o_s.at[near], recv_sem=o_r.at[off_o], device_id={"sp": to}, device_id_type=MESH)

    def fold(block, op):
        return op(block.reshape(block.shape[0] // 8, 8, block.shape[1]), axis=0)

    def attend(i):
        idx = n_chip - 1 - i
        off_q = offset_of(idx)
        src = lax.rem(chip + n_chip - off_q, n_chip)
        off_o = lax.rem(n_chip - off_q, n_chip)

        @pl.when(i > 0)
        def _():
            with jax.named_scope("q_arrive"):
                exchange(0, idx).wait_recv()

        src_at = pl.ds(pl.multiple_of(src * rows, rows), rows)
        causal = lax.broadcasted_iota(jnp.int32, (rows, rows), 0) <= lax.broadcasted_iota(jnp.int32, (rows, rows), 1)
        blocks = [slice(kb * rows, (kb + 1) * rows) for kb in range(n_chip)]
        tops = []
        for h in range(heads):
            at = slice(h * HEAD_DIM, (h + 1) * HEAD_DIM)
            sc = lax.dot_general(recv[1, :, at], recv[0, src_at, at], contract_last, preferred_element_type=F32)
            s_ref[h] = sc
            top = jnp.full((8, rows), -jnp.inf, F32)
            for kb in range(n_chip):
                top = jnp.maximum(top, fold(sc[blocks[kb]], jnp.max) + jnp.where(kb < src, 0.0, -jnp.inf))
            tops.append(top)
        for h in range(heads):
            at = slice(h * HEAD_DIM, (h + 1) * HEAD_DIM)
            own = jnp.where(causal, s_ref[h, src_at, :], -jnp.inf)
            s_ref[h, src_at, :] = own
            top = jnp.max(jnp.maximum(tops[h], fold(own, jnp.max)), axis=0, keepdims=True) * log_scale
            total = jnp.zeros((8, rows), F32)
            for kb in range(n_chip):
                ex = jnp.exp2(s_ref[h, blocks[kb], :] * log_scale + (jnp.where(kb <= src, 0.0, -jnp.inf) - top))
                s_ref[h, blocks[kb], :] = ex
                total = total + fold(ex, jnp.sum)
            inv = 1.0 / jnp.sum(total, axis=0, keepdims=True)
            for kb in range(n_chip):
                p_ref[h, blocks[kb], :] = (s_ref[h, blocks[kb], :] * inv).astype(BF16)
            osend[i, :, at] = jnp.dot(vt[h], p_ref[h], preferred_element_type=F32).T.astype(BF16)

        @pl.when(i > 0)
        def _():
            for kk in range(2):
                o_copy(i, kk, 2 * src + kk, off_o).start()

        @pl.when(i == 0)
        def _():
            o_copy(i, 1 - core, sibling, off_o, 1).start()
            orecv[0, pl.ds(0, tok), pl.ds(pl.multiple_of(core * cols, cols), cols)] = osend[0, my_rows, :]

    zero_half = jnp.zeros((8, cols), BF16)

    def gather(i):
        off_o = lax.rem(n_chip - offset_of(n_chip - 1 - i), n_chip)
        src = lax.rem(chip + n_chip - off_o, n_chip)

        def arrived(span):
            at = (off_o, pl.ds(0, tok), span)
            pltpu.make_async_remote_copy(
                src_ref=orecv.at[at], dst_ref=orecv.at[at], send_sem=o_s.at[0], recv_sem=o_r.at[off_o],
                device_id={"sp": sibling}, device_id_type=MESH).wait_recv()

        @pl.when(i == 0)
        def _():
            d_whole().wait_recv()
            arrived(pl.ds(pl.multiple_of((1 - core) * cols, cols), cols))

        @pl.when(i > 0)
        def _():
            with jax.named_scope("o_arrive"):
                arrived(pl.ds(0, wide))

        d0 = jnp.broadcast_to(dsum[2 * off_o].astype(BF16), (8, cols))
        d1 = jnp.broadcast_to(dsum[2 * off_o + 1].astype(BF16), (8, cols))
        orecv[off_o, pl.ds(tok, PAD), :] = jnp.concatenate(
            [jnp.concatenate([d0, zero_half], axis=1), jnp.concatenate([zero_half, d1], axis=1)], axis=0)
        k_at = pl.ds(pl.multiple_of(src * wide, wide), wide)
        lhs = orecv[off_o]
        for j in range(n_wo):
            res = jnp.dot(lhs, pool[j, k_at, :], preferred_element_type=F32)
            parts = res[tok:tok + 8].astype(BF16).astype(F32) + res[tok + 8:].astype(BF16).astype(F32)
            n_at = slice(j * wide, (j + 1) * wide)
            acc[pl.ds(0, tok), n_at] += res[:tok]
            acc[pl.ds(tok, 8), n_at] += parts

    def drain_early():
        x_send.wait_send()
        for t in range(2):
            pltpu.make_async_remote_copy(
                src_ref=ssq.at[t], dst_ref=ssq_in.at[t], send_sem=ss_s.at[t], recv_sem=ss_r.at[t],
                device_id={"sp": sibling}, device_id_type=MESH).wait_send()

        for t in range(3):
            whole(t).wait_send()
        d_whole().wait_send()

    def both(i, carry):
        @pl.when(i < n_chip)
        def _():
            with jax.named_scope("attend"):
                attend(i)

        @pl.when(i == LAG)
        def _():
            pltpu.make_async_copy(pool, pool, wosem).wait()
            drain_early()

        @pl.when(i >= LAG)
        def _():
            with jax.named_scope("gather"):
                gather(i - LAG)
        return carry

    lax.fori_loop(0, n_chip + LAG, both, 0)

    def finish(r):
        r_at = pl.ds(r * PAD, PAD)
        val = acc[r_at, :]
        scale = lax.rsqrt(jnp.sum(val * val, axis=1, keepdims=True) * (1.0 / width) + NORM_EPS)
        x_at = pl.ds(pl.multiple_of(core * tok + r * PAD, PAD), PAD)
        outp_ref[r_at, :] = (xs[x_at, :].astype(F32) + val * scale * gains[2]).astype(BF16)

    with jax.named_scope("finish"):
        for r in range(tok // PAD):
            finish(r)
        val = acc[pl.ds(tok, 8), :]
        scale = lax.rsqrt(jnp.sum(val * val, axis=1, keepdims=True) * (1.0 / width) + NORM_EPS)
        outd_ref[...] = (new_ref[...].astype(F32) + (val * scale * gains[2])[0:1]).astype(BF16)

    o_copy(0, 1 - core, sibling, 0, 1).wait_send()
    far = osend.at[pl.ds(1, n_chip - 1)]
    pltpu.make_async_remote_copy(
        src_ref=far, dst_ref=far, send_sem=o_s.at[0], recv_sem=o_r.at[0],
        device_id={"sp": sibling}, device_id_type=MESH).wait_send()


def hand_over(outp_in, kc_in, vc_in, outd_in, outp, kc, vc, outd, sem):
    outs = [pltpu.make_async_copy(a, b, sem.at[n]) for n, (a, b) in enumerate(
        ((outp_in, outp), (kc_in, kc.reshape(kc_in.shape)), (vc_in, vc.reshape(vc_in.shape)), (outd_in, outd)))]
    for one in outs:
        one.start()
    for one in outs:
        one.wait()


def solution(mesh):
    n_dev = mesh.shape["sp"]

    def device_step(prompt_blk, w_q, w_k, w_v, w_o, q_norm_w, k_norm_w, post_norm_w, new_rows):
        _, tok, width = prompt_blk.shape
        n_chip = n_dev // 2
        rows, seq, cols = 2 * tok, tok * n_dev, width // n_dev
        heads = cols // HEAD_DIM
        wide = 2 * cols
        n_wo = width // wide
        table = jnp.asarray(rope_table(seq))
        hbm = pl.BlockSpec(memory_space=pltpu.HBM)
        vmem = pl.BlockSpec(memory_space=pltpu.VMEM)
        dma = pltpu.SemaphoreType.DMA
        cache_shape = jax.ShapeDtypeStruct((heads * (seq + 1), HEAD_DIM), BF16)

        def keep(value):
            return pltpu.with_memory_space_constraint(value, pltpu.HBM)

        outp, kc, vc, outd = pl.pallas_call(
            functools.partial(kernel, n_dev),
            out_shape=(jax.ShapeDtypeStruct((tok, width), BF16), cache_shape, cache_shape, jax.ShapeDtypeStruct((1, width), BF16)),
            in_specs=[hbm] * 10,
            out_specs=(vmem,) * 4,
            scratch_shapes=[
                pltpu.VMEM((1, width), BF16),
                pltpu.VMEM((3, 1, width), F32),
                pltpu.VMEM((rows + PAD, width), BF16),
                pltpu.VMEM((n_wo, width, wide), BF16),
                pltpu.VMEM((rows + PAD, HEAD_DIM), F32),
                pltpu.VMEM((n_chip, rows + PAD, cols), F32),
                pltpu.VMEM((2, rows + PAD, HEAD_DIM), F32),
                pltpu.VMEM((2, rows + PAD, HEAD_DIM), F32),
                pltpu.VMEM((3, n_chip, rows, cols), BF16),
                pltpu.VMEM((3, seq, cols), BF16),
                pltpu.VMEM((3, PAD, cols), BF16),
                pltpu.VMEM((heads, seq, rows), F32),
                pltpu.VMEM((heads, seq, rows), BF16),
                pltpu.VMEM((heads, HEAD_DIM, seq), BF16),
                pltpu.VMEM((n_chip, rows, cols), BF16),
                pltpu.VMEM((n_chip, tok + PAD, wide), BF16),
                pltpu.VMEM((1, cols), F32),
                pltpu.VMEM((n_dev, 1, cols), F32),
                pltpu.VMEM((tok + 8, width), F32),
                pltpu.VMEM((heads * rows, HEAD_DIM), F32),
                dma(()), dma((2,)), dma((n_chip // 2,)), dma(()), dma(()),
                dma(()), dma(()), dma((2,)), dma((2,)),
                dma((3,)), dma((3,)), dma((n_chip,)),
                dma(()), dma(()),
                dma((2,)), dma((n_chip,)),
            ],
            compiler_params=pltpu.CompilerParams(collective_id=0, has_side_effects=True, vmem_limit_bytes=VMEM_MIB * 1024 * 1024),
        )(keep(prompt_blk[0]), keep(new_rows), w_q, w_k, w_v, w_o, keep(q_norm_w[None]), keep(k_norm_w[None]), keep(post_norm_w[None]), keep(table))
        shape = (seq + 1, heads, HEAD_DIM)
        outs = pl.pallas_call(
            hand_over,
            out_shape=(jax.ShapeDtypeStruct((tok, width), BF16), jax.ShapeDtypeStruct(shape, BF16),
                       jax.ShapeDtypeStruct(shape, BF16), jax.ShapeDtypeStruct((1, width), BF16)),
            in_specs=[vmem] * 4,
            out_specs=(hbm,) * 4,
            scratch_shapes=[dma((4,))],
            compiler_params=pltpu.CompilerParams(vmem_limit_bytes=8 * 1024 * 1024),
        )(outp, kc, vc, outd)
        return outs[0][None], outs[1][None], outs[2][None], outs[3]

    replicated = P()
    return jax.shard_map(
        device_step, mesh=mesh,
        in_specs=(P("dp", "sp", None), replicated, replicated, replicated, replicated, replicated, replicated, replicated, P("dp", None)),
        out_specs=(P("dp", "sp", None), P("dp", None, "sp", None), P("dp", None, "sp", None), P("dp", None)),
        check_vma=False)
```

```python
import functools
import math

import jax
import jax.numpy as jnp
import numpy as np
from jax import lax
from jax.experimental import pallas as pl
from jax.experimental.pallas import tpu as pltpu
from jax.sharding import PartitionSpec as P

HEAD_DIM = 128
ROPE_THETA = 500000.0
NORM_EPS = 1e-6
PAD = 16
VMEM_MIB = 50
LAG = 6
MASKED = -1e30
F32 = jnp.float32
BF16 = jnp.bfloat16
MESH = pl.DeviceIdType.MESH


def rope_table(seq_len):
    half = HEAD_DIM // 2
    inv_freq = np.power(np.float32(ROPE_THETA), -np.arange(0, HEAD_DIM, 2).astype(np.float32) / np.float32(HEAD_DIM)).astype(np.float32)
    pos = np.minimum(np.arange(seq_len + PAD), seq_len).astype(np.float32)
    angles = (pos[:, None] * inv_freq[None, :half]).astype(np.float32)
    return np.concatenate([np.cos(angles), np.sin(angles)], axis=-1).astype(np.float32)


def kernel(n_dev, x_hbm, new_hbm, wq, wk, wv, wo, qg_hbm, kg_hbm, pg_hbm, tab_hbm,
           outp_ref, kc_ref, vc_ref, outd_ref,
           new_ref, gains,
           xs, pool, tab, raw, ssq, ssq_in, send, recv, new, s_ref, p_ref, vt, osend, orecv, dsend, dsum, acc, stage,
           xsem, insem, wfirst, wsem, wosem, tabsem, xs_s, xs_r, ss_s, ss_r, a_s, a_r, q_r, d_s, d_r, o_s, o_r):
    tok = x_hbm.shape[0]
    width = x_hbm.shape[1]
    rows = 2 * tok
    n_chip = n_dev // 2
    half_chip = n_chip // 2
    cols = width // n_dev
    heads = cols // HEAD_DIM
    seq = tok * n_dev
    n_step = n_chip // 2
    n_wo = pool.shape[0]
    wide = 2 * cols

    me = lax.axis_index("sp")
    chip = lax.div(me, 2)
    core = lax.rem(me, 2)
    sibling = 2 * chip + (1 - core)

    def offset_of(idx):
        odd = lax.rem(idx, 2)
        return lax.rem(half_chip + odd + (2 * odd - 1) * lax.div(idx, 2), n_chip)

    def group_col(idx):
        dest = lax.rem(chip + offset_of(idx), n_chip)
        return pl.multiple_of((2 * dest + core) * cols, cols)

    def w_copy(w_ref, s, half):
        return pltpu.make_async_copy(
            w_ref.at[:, pl.ds(group_col(2 * s + half), cols)], pool.at[s, :, pl.ds(half * cols, cols)], wsem.at[s])

    def w_wait(s):
        pltpu.make_async_copy(pool.at[s], pool.at[s], wsem.at[s]).wait()

    depth = width // 2

    def w_first(part, half):
        d_at = pl.ds(part * depth, depth)
        return pltpu.make_async_copy(
            wv.at[d_at, pl.ds(group_col(half), cols)], pool.at[0, d_at, pl.ds(half * cols, cols)], wfirst.at[part])

    def wo_copy(j):
        return pltpu.make_async_copy(wo.at[:, pl.ds(pl.multiple_of(j * wide, wide), wide)], pool.at[j], wosem)

    my_rows = pl.ds(pl.multiple_of(core * tok, tok), tok)
    x_copy = pltpu.make_async_copy(x_hbm, xs.at[my_rows], xsem)
    x_copy.start()
    smalls = [pltpu.make_async_copy(a, b, insem.at[n]) for a, b, n in (
        (new_hbm, new_ref, 0), (qg_hbm, gains.at[0], 1), (kg_hbm, gains.at[1], 1), (pg_hbm, gains.at[2], 1))]
    for part in range(2):
        for half in range(2):
            w_first(part, half).start()
    barrier = pltpu.get_barrier_semaphore()
    for off in sorted(range(1, n_dev), key=lambda off: -min(off, n_dev - off)):
        pl.semaphore_signal(barrier, inc=1, device_id={"sp": lax.rem(me + off, n_dev)}, device_id_type=MESH)

    for small in smalls:
        small.start()
    tab_a = pltpu.make_async_copy(tab_hbm.at[pl.ds(pl.multiple_of(chip * rows, rows), rows)], tab.at[pl.ds(0, rows)], tabsem)
    tab_b = pltpu.make_async_copy(tab_hbm.at[pl.ds(seq, PAD)], tab.at[pl.ds(rows, PAD)], tabsem)
    tab_a.start()
    tab_b.start()

    x_copy.wait()
    for s in range(1, n_step):
        w_copy(wv, s, 0).start()
        w_copy(wv, s, 1).start()

    own_rows = pl.ds(pl.multiple_of(chip * rows, rows), rows)

    def exchange(t, idx):
        dest = lax.rem(chip + offset_of(idx), n_chip)
        return pltpu.make_async_remote_copy(
            src_ref=send.at[t, idx], dst_ref=recv.at[t, own_rows], send_sem=a_s.at[t], recv_sem=a_r.at[t] if t else q_r.at[idx],
            device_id={"sp": 2 * dest + core}, device_id_type=MESH)

    def emit(t, idx, block):
        @pl.when(idx < n_chip - 1)
        def _():
            send[t, idx] = block[:rows]
            exchange(t, idx).start()

        @pl.when(idx == n_chip - 1)
        def _():
            recv[t, own_rows, :] = block[:rows]
            new[t] = block[rows:]

    def project(s):
        w_wait(s)
        return jnp.dot(xs[...], pool[s], preferred_element_type=F32)

    def half_exchange(idx, which):
        dest = lax.rem(chip + offset_of(idx), n_chip)
        at = pl.ds(pl.multiple_of(which * tok, tok), tok)
        return pltpu.make_async_remote_copy(
            src_ref=send.at[2, idx, at], dst_ref=recv.at[2, pl.ds(pl.multiple_of(chip * rows + which * tok, tok), tok)],
            send_sem=a_s.at[2], recv_sem=a_r.at[2], device_id={"sp": 2 * dest + core}, device_id_type=MESH)

    def half_project(which, res=None):
        at = pl.ds(pl.multiple_of(which * tok, tok), tok)
        if res is None:
            res = jnp.dot(xs[at, :], pool[0], preferred_element_type=F32)
        res = res.astype(BF16)
        for idx in range(2):
            send[2, idx, at, :] = res[:, idx * cols:(idx + 1) * cols]

    res = None
    for part in range(2):
        d_at = pl.ds(part * depth, depth)
        pltpu.make_async_copy(pool.at[0, d_at], pool.at[0, d_at], wfirst.at[part]).wait()
        with jax.named_scope("v_first"):
            piece = jnp.dot(xs[my_rows, d_at], pool[0, d_at, :], preferred_element_type=F32)
            res = piece if res is None else res + piece
    half_project(core, res)
    with jax.named_scope("barrier"):
        pl.semaphore_wait(barrier, n_dev - 1)
    x_send = pltpu.make_async_remote_copy(
        src_ref=xs.at[my_rows], dst_ref=xs.at[my_rows], send_sem=xs_s, recv_sem=xs_r, device_id={"sp": sibling}, device_id_type=MESH)
    x_send.start()
    for idx in range(2):
        half_exchange(idx, core).start()
    smalls[0].wait()
    pltpu.make_async_copy(gains, gains, insem.at[1]).wait()
    xs[pl.ds(rows, PAD), :] = jnp.broadcast_to(new_ref[...], (PAD, width))
    acc[...] = jnp.zeros_like(acc)
    with jax.named_scope("x_arrive"):
        x_send.wait_recv()

    def v_step(s, carry):
        res = project(s)
        w_copy(wk, s, 0).start()
        w_copy(wk, s, 1).start()
        for half in range(2):
            emit(2, 2 * s + half, res[:, half * cols:(half + 1) * cols].astype(BF16))
        return carry

    with jax.named_scope('v_proj'):
        lax.fori_loop(1, n_step, v_step, 0)
        half_project(1 - core)
        for idx in range(2):
            half_exchange(idx, 1 - core).start()
        w_copy(wk, 0, 0).start()
        w_copy(wk, 0, 1).start()
    pltpu.make_async_copy(tab, tab, tabsem).wait()

    lane = lax.broadcasted_iota(jnp.int32, (rows + PAD, HEAD_DIM), 1)
    first = lane < HEAD_DIM // 2

    def raw_step(t, i):
        s = lax.rem(i + 1, n_step)
        res = project(s)
        sq = jnp.zeros((rows + PAD, HEAD_DIM), F32)
        for half in range(2):
            part = res[:, half * cols:(half + 1) * cols]
            raw[2 * s + half] = part
            for h in range(heads):
                piece = part[:, h * HEAD_DIM:(h + 1) * HEAD_DIM]
                sq = sq + piece * piece
        @pl.when(i == 0)
        def _():
            ssq[t] = sq

        @pl.when(i > 0)
        def _():
            ssq[t] += sq

        return s

    def norm_and_send(t, g_ref):
        swap = pltpu.make_async_remote_copy(
            src_ref=ssq.at[t], dst_ref=ssq_in.at[t], send_sem=ss_s.at[t], recv_sem=ss_r.at[t],
            device_id={"sp": sibling}, device_id_type=MESH)
        swap.start()
        swap.wait_recv()
        total = jnp.sum(ssq[t] + ssq_in[t], axis=1, keepdims=True)
        scale = lax.rsqrt(total * (1.0 / width) + NORM_EPS)

        def one(n, carry):
            idx = n if t else n_chip - 1 - n
            g = g_ref[:, pl.ds(group_col(idx), cols)]
            table = tab[...]
            turned = pltpu.roll(table, HEAD_DIM // 2, 1)
            cos = jnp.where(first, table, turned)
            sin = jnp.where(first, -turned, table)
            parts = []
            for h in range(heads):
                at = slice(h * HEAD_DIM, (h + 1) * HEAD_DIM)
                val = raw[idx, :, at] * scale * g[:, at]
                parts.append((val * cos + pltpu.roll(val, HEAD_DIM // 2, 1) * sin).astype(BF16))
            emit(t, idx, jnp.concatenate(parts, axis=1))
            return carry

        lax.fori_loop(0, n_chip, one, 0)

    def k_step(i, carry):
        s = raw_step(1, i)
        w_copy(wq, s, 0).start()
        w_copy(wq, s, 1).start()
        return carry

    with jax.named_scope('k_proj'):
        lax.fori_loop(0, n_step, k_step, 0)
    with jax.named_scope('k_norm'):
        norm_and_send(1, gains.at[1])
    for j in range(n_step, n_wo):
        wo_copy(j).start()

    def q_step(i, carry):
        s = raw_step(0, i)
        wo_copy(s).start()
        return carry

    with jax.named_scope('q_proj'):
        lax.fori_loop(0, n_step, q_step, 0)
    with jax.named_scope('q_norm'):
        norm_and_send(0, gains.at[0])

    def whole(t):
        every = pl.ds(0, (n_chip - 1) * rows)
        return pltpu.make_async_remote_copy(
            src_ref=recv.at[t, every], dst_ref=recv.at[t, every], send_sem=a_s.at[t], recv_sem=a_r.at[t],
            device_id={"sp": sibling}, device_id_type=MESH)

    def fill_cache(t, cache):
        def one(b, carry):
            base = pl.multiple_of(b * rows, rows)
            block = recv[t, pl.ds(base, rows), :].astype(F32)
            for h in range(heads):
                stage[pl.ds(h, rows, stride=heads), :] = block[:, h * HEAD_DIM:(h + 1) * HEAD_DIM]
            cache[pl.ds(pl.multiple_of(heads * base, heads * rows), heads * rows), :] = stage[...].astype(BF16)
            return carry
        lax.fori_loop(0, n_chip, one, 0)
        last = new[t][0:1, :].astype(F32)
        rows_new = jnp.concatenate([last[:, h * HEAD_DIM:(h + 1) * HEAD_DIM] for h in range(heads)], axis=0)
        cache[pl.ds(heads * seq, heads), :] = rows_new.astype(BF16)

    with jax.named_scope("v_arrive"):
        whole(2).wait_recv()
    with jax.named_scope("v_cache"):
        fill_cache(2, vc_ref)
        for b in range(n_chip):
            for h in range(heads):
                vt[h, :, b * rows:(b + 1) * rows] = recv[2, b * rows:(b + 1) * rows, h * HEAD_DIM:(h + 1) * HEAD_DIM].astype(F32).T.astype(BF16)
    with jax.named_scope("k_arrive"):
        whole(1).wait_recv()
    with jax.named_scope("k_cache"):
        fill_cache(1, kc_ref)

    log_scale = HEAD_DIM ** -0.5 * math.log2(math.e)
    contract_last = (((1,), (1,)), ((), ()))

    for h in range(heads):
        at = slice(h * HEAD_DIM, (h + 1) * HEAD_DIM)
        qd, kd, vd = new[0][:, at], new[1][:, at], new[2][:, at]
        sc = lax.dot_general(qd, recv[1, :, at], contract_last, preferred_element_type=F32) * log_scale
        sn = jnp.sum(qd.astype(F32) * kd.astype(F32), axis=1, keepdims=True) * log_scale
        top = jnp.maximum(jnp.max(sc, axis=1, keepdims=True), sn)
        ex = jnp.exp2(sc - top)
        en = jnp.exp2(sn - top)
        inv = 1.0 / (jnp.sum(ex, axis=1, keepdims=True) + en)
        prob = (ex * inv).astype(BF16)
        prob_n = (en * inv).astype(BF16).astype(F32)
        od = jnp.dot(prob, recv[2, :, at], preferred_element_type=F32) + prob_n * vd.astype(F32)
        dsend[:, at] = od[0:1].astype(BF16).astype(F32)

    def d_copy(off, to):
        return pltpu.make_async_remote_copy(
            src_ref=dsend, dst_ref=dsum.at[2 * off + core], send_sem=d_s, recv_sem=d_r,
            device_id={"sp": to}, device_id_type=MESH)

    d_copy(0, sibling).start()
    for off in range(1, n_chip):
        for kk in range(2):
            d_copy(off, 2 * lax.rem(chip + off, n_chip) + kk).start()
    dsum[core] = dsend[...]

    def d_whole():
        every = pl.ds(0, n_dev - 1)
        return pltpu.make_async_remote_copy(
            src_ref=dsum.at[every], dst_ref=dsum.at[every], send_sem=d_s, recv_sem=d_r,
            device_id={"sp": sibling}, device_id_type=MESH)

    def o_copy(i, kk, to, off_o, near=0):
        return pltpu.make_async_remote_copy(
            src_ref=osend.at[i, pl.ds(pl.multiple_of(kk * tok, tok), tok)],
            dst_ref=orecv.at[off_o, pl.ds(0, tok), pl.ds(pl.multiple_of(core * cols, cols), cols)],
            send_sem=o_s.at[near], recv_sem=o_r.at[off_o], device_id={"sp": to}, device_id_type=MESH)

    def fold(block, op):
        return op(block.reshape(block.shape[0] // 8, 8, block.shape[1]), axis=0)

    def attend(i):
        idx = n_chip - 1 - i
        off_q = offset_of(idx)
        src = lax.rem(chip + n_chip - off_q, n_chip)
        off_o = lax.rem(n_chip - off_q, n_chip)

        @pl.when(i > 0)
        def _():
            with jax.named_scope("q_arrive"):
                exchange(0, idx).wait_recv()

        src_at = pl.ds(pl.multiple_of(src * rows, rows), rows)
        causal = lax.broadcasted_iota(jnp.int32, (rows, rows), 0) <= lax.broadcasted_iota(jnp.int32, (rows, rows), 1)
        blocks = [slice(kb * rows, (kb + 1) * rows) for kb in range(n_chip)]
        tops = []
        for h in range(heads):
            at = slice(h * HEAD_DIM, (h + 1) * HEAD_DIM)
            sc = lax.dot_general(recv[1, :, at], recv[0, src_at, at], contract_last, preferred_element_type=F32)
            s_ref[h] = sc
            top = jnp.full((8, rows), -jnp.inf, F32)
            for kb in range(n_chip):
                top = jnp.maximum(top, fold(sc[blocks[kb]], jnp.max) + jnp.where(kb < src, 0.0, -jnp.inf))
            tops.append(top)
        for h in range(heads):
            at = slice(h * HEAD_DIM, (h + 1) * HEAD_DIM)
            own = jnp.where(causal, s_ref[h, src_at, :], -jnp.inf)
            s_ref[h, src_at, :] = own
            top = jnp.max(jnp.maximum(tops[h], fold(own, jnp.max)), axis=0, keepdims=True) * log_scale
            total = jnp.zeros((8, rows), F32)
            for kb in range(n_chip):
                ex = jnp.exp2(s_ref[h, blocks[kb], :] * log_scale + (jnp.where(kb <= src, 0.0, -jnp.inf) - top))
                s_ref[h, blocks[kb], :] = ex
                total = total + fold(ex, jnp.sum)
            inv = 1.0 / jnp.sum(total, axis=0, keepdims=True)
            for kb in range(n_chip):
                p_ref[h, blocks[kb], :] = (s_ref[h, blocks[kb], :] * inv).astype(BF16)
            osend[i, :, at] = jnp.dot(vt[h], p_ref[h], preferred_element_type=F32).T.astype(BF16)

        @pl.when(i > 0)
        def _():
            for kk in range(2):
                o_copy(i, kk, 2 * src + kk, off_o).start()

        @pl.when(i == 0)
        def _():
            o_copy(i, 1 - core, sibling, off_o, 1).start()
            orecv[0, pl.ds(0, tok), pl.ds(pl.multiple_of(core * cols, cols), cols)] = osend[0, my_rows, :]

    zero_half = jnp.zeros((8, cols), BF16)

    def gather(i):
        off_o = lax.rem(n_chip - offset_of(n_chip - 1 - i), n_chip)
        src = lax.rem(chip + n_chip - off_o, n_chip)

        def arrived(span):
            at = (off_o, pl.ds(0, tok), span)
            pltpu.make_async_remote_copy(
                src_ref=orecv.at[at], dst_ref=orecv.at[at], send_sem=o_s.at[0], recv_sem=o_r.at[off_o],
                device_id={"sp": sibling}, device_id_type=MESH).wait_recv()

        @pl.when(i == 0)
        def _():
            d_whole().wait_recv()
            arrived(pl.ds(pl.multiple_of((1 - core) * cols, cols), cols))

        @pl.when(i > 0)
        def _():
            with jax.named_scope("o_arrive"):
                arrived(pl.ds(0, wide))

        d0 = jnp.broadcast_to(dsum[2 * off_o].astype(BF16), (8, cols))
        d1 = jnp.broadcast_to(dsum[2 * off_o + 1].astype(BF16), (8, cols))
        orecv[off_o, pl.ds(tok, PAD), :] = jnp.concatenate(
            [jnp.concatenate([d0, zero_half], axis=1), jnp.concatenate([zero_half, d1], axis=1)], axis=0)
        k_at = pl.ds(pl.multiple_of(src * wide, wide), wide)
        lhs = orecv[off_o]
        for j in range(n_wo):
            res = jnp.dot(lhs, pool[j, k_at, :], preferred_element_type=F32)
            parts = res[tok:tok + 8].astype(BF16).astype(F32) + res[tok + 8:].astype(BF16).astype(F32)
            n_at = slice(j * wide, (j + 1) * wide)
            acc[pl.ds(0, tok), n_at] += res[:tok]
            acc[pl.ds(tok, 8), n_at] += parts

    def drain_early():
        x_send.wait_send()
        for t in range(2):
            pltpu.make_async_remote_copy(
                src_ref=ssq.at[t], dst_ref=ssq_in.at[t], send_sem=ss_s.at[t], recv_sem=ss_r.at[t],
                device_id={"sp": sibling}, device_id_type=MESH).wait_send()

        for t in range(3):
            whole(t).wait_send()
        d_whole().wait_send()

    def both(i, carry):
        @pl.when(i < n_chip)
        def _():
            with jax.named_scope("attend"):
                attend(i)

        @pl.when(i == LAG)
        def _():
            pltpu.make_async_copy(pool, pool, wosem).wait()
            drain_early()

        @pl.when(i >= LAG)
        def _():
            with jax.named_scope("gather"):
                gather(i - LAG)
        return carry

    lax.fori_loop(0, n_chip + LAG, both, 0)

    def finish(r):
        r_at = pl.ds(r * PAD, PAD)
        val = acc[r_at, :]
        scale = lax.rsqrt(jnp.sum(val * val, axis=1, keepdims=True) * (1.0 / width) + NORM_EPS)
        x_at = pl.ds(pl.multiple_of(core * tok + r * PAD, PAD), PAD)
        outp_ref[r_at, :] = (xs[x_at, :].astype(F32) + val * scale * gains[2]).astype(BF16)

    with jax.named_scope("finish"):
        for r in range(tok // PAD):
            finish(r)
        val = acc[pl.ds(tok, 8), :]
        scale = lax.rsqrt(jnp.sum(val * val, axis=1, keepdims=True) * (1.0 / width) + NORM_EPS)
        outd_ref[...] = (new_ref[...].astype(F32) + (val * scale * gains[2])[0:1]).astype(BF16)

    o_copy(0, 1 - core, sibling, 0, 1).wait_send()
    far = osend.at[pl.ds(1, n_chip - 1)]
    pltpu.make_async_remote_copy(
        src_ref=far, dst_ref=far, send_sem=o_s.at[0], recv_sem=o_r.at[0],
        device_id={"sp": sibling}, device_id_type=MESH).wait_send()


def hand_over(outp_in, kc_in, vc_in, outd_in, outp, kc, vc, outd, sem):
    outs = [pltpu.make_async_copy(a, b, sem.at[n]) for n, (a, b) in enumerate(
        ((outp_in, outp), (kc_in, kc.reshape(kc_in.shape)), (vc_in, vc.reshape(vc_in.shape)), (outd_in, outd)))]
    for one in outs:
        one.start()
    for one in outs:
        one.wait()


def solution(mesh):
    n_dev = mesh.shape["sp"]

    def device_step(prompt_blk, w_q, w_k, w_v, w_o, q_norm_w, k_norm_w, post_norm_w, new_rows):
        _, tok, width = prompt_blk.shape
        n_chip = n_dev // 2
        rows, seq, cols = 2 * tok, tok * n_dev, width // n_dev
        heads = cols // HEAD_DIM
        wide = 2 * cols
        n_wo = width // wide
        table = jnp.asarray(rope_table(seq))
        hbm = pl.BlockSpec(memory_space=pltpu.HBM)
        vmem = pl.BlockSpec(memory_space=pltpu.VMEM)
        dma = pltpu.SemaphoreType.DMA
        cache_shape = jax.ShapeDtypeStruct((heads * (seq + 1), HEAD_DIM), BF16)

        def keep(value):
            return pltpu.with_memory_space_constraint(value, pltpu.HBM)

        outp, kc, vc, outd = pl.pallas_call(
            functools.partial(kernel, n_dev),
            out_shape=(jax.ShapeDtypeStruct((tok, width), BF16), cache_shape, cache_shape, jax.ShapeDtypeStruct((1, width), BF16)),
            in_specs=[hbm] * 10,
            out_specs=(vmem,) * 4,
            scratch_shapes=[
                pltpu.VMEM((1, width), BF16),
                pltpu.VMEM((3, 1, width), F32),
                pltpu.VMEM((rows + PAD, width), BF16),
                pltpu.VMEM((n_wo, width, wide), BF16),
                pltpu.VMEM((rows + PAD, HEAD_DIM), F32),
                pltpu.VMEM((n_chip, rows + PAD, cols), F32),
                pltpu.VMEM((2, rows + PAD, HEAD_DIM), F32),
                pltpu.VMEM((2, rows + PAD, HEAD_DIM), F32),
                pltpu.VMEM((3, n_chip, rows, cols), BF16),
                pltpu.VMEM((3, seq, cols), BF16),
                pltpu.VMEM((3, PAD, cols), BF16),
                pltpu.VMEM((heads, seq, rows), F32),
                pltpu.VMEM((heads, seq, rows), BF16),
                pltpu.VMEM((heads, HEAD_DIM, seq), BF16),
                pltpu.VMEM((n_chip, rows, cols), BF16),
                pltpu.VMEM((n_chip, tok + PAD, wide), BF16),
                pltpu.VMEM((1, cols), F32),
                pltpu.VMEM((n_dev, 1, cols), F32),
                pltpu.VMEM((tok + 8, width), F32),
                pltpu.VMEM((heads * rows, HEAD_DIM), F32),
                dma(()), dma((2,)), dma((2,)), dma((n_chip // 2,)), dma(()), dma(()),
                dma(()), dma(()), dma((2,)), dma((2,)),
                dma((3,)), dma((3,)), dma((n_chip,)),
                dma(()), dma(()),
                dma((2,)), dma((n_chip,)),
            ],
            compiler_params=pltpu.CompilerParams(collective_id=0, has_side_effects=True, vmem_limit_bytes=VMEM_MIB * 1024 * 1024),
        )(keep(prompt_blk[0]), keep(new_rows), w_q, w_k, w_v, w_o, keep(q_norm_w[None]), keep(k_norm_w[None]), keep(post_norm_w[None]), keep(table))
        shape = (seq + 1, heads, HEAD_DIM)
        outs = pl.pallas_call(
            hand_over,
            out_shape=(jax.ShapeDtypeStruct((tok, width), BF16), jax.ShapeDtypeStruct(shape, BF16),
                       jax.ShapeDtypeStruct(shape, BF16), jax.ShapeDtypeStruct((1, width), BF16)),
            in_specs=[vmem] * 4,
            out_specs=(hbm,) * 4,
            scratch_shapes=[dma((4,))],
            compiler_params=pltpu.CompilerParams(vmem_limit_bytes=8 * 1024 * 1024),
        )(outp, kc, vc, outd)
        return outs[0][None], outs[1][None], outs[2][None], outs[3]

    replicated = P()
    return jax.shard_map(
        device_step, mesh=mesh,
        in_specs=(P("dp", "sp", None), replicated, replicated, replicated, replicated, replicated, replicated, replicated, P("dp", None)),
        out_specs=(P("dp", "sp", None), P("dp", None, "sp", None), P("dp", None, "sp", None), P("dp", None)),
        check_vma=False)
```

```python
import functools
import math

import jax
import jax.numpy as jnp
import numpy as np
from jax import lax
from jax.experimental import pallas as pl
from jax.experimental.pallas import tpu as pltpu
from jax.sharding import PartitionSpec as P

HEAD_DIM = 128
ROPE_THETA = 500000.0
NORM_EPS = 1e-6
PAD = 16
VMEM_MIB = 50
LAG = 8
MASKED = -1e30
F32 = jnp.float32
BF16 = jnp.bfloat16
MESH = pl.DeviceIdType.MESH


def rope_table(seq_len):
    half = HEAD_DIM // 2
    inv_freq = np.power(np.float32(ROPE_THETA), -np.arange(0, HEAD_DIM, 2).astype(np.float32) / np.float32(HEAD_DIM)).astype(np.float32)
    pos = np.minimum(np.arange(seq_len + PAD), seq_len).astype(np.float32)
    angles = (pos[:, None] * inv_freq[None, :half]).astype(np.float32)
    return np.concatenate([np.cos(angles), np.sin(angles)], axis=-1).astype(np.float32)


def kernel(n_dev, x_hbm, new_hbm, wq, wk, wv, wo, qg_hbm, kg_hbm, pg_hbm, tab_hbm,
           outp_ref, kc_ref, vc_ref, outd_ref,
           new_ref, gains,
           xs, pool, tab, raw, ssq, ssq_in, send, recv, new, s_ref, p_ref, vt, osend, orecv, dsend, dsum, acc, stage,
           xsem, insem, wsem, wosem, tabsem, xs_s, xs_r, ss_s, ss_r, a_s, a_r, q_r, d_s, d_r, o_s, o_r):
    tok = x_hbm.shape[0]
    width = x_hbm.shape[1]
    rows = 2 * tok
    n_chip = n_dev // 2
    half_chip = n_chip // 2
    cols = width // n_dev
    heads = cols // HEAD_DIM
    seq = tok * n_dev
    n_step = n_chip // 2
    n_wo = pool.shape[0]
    wide = 2 * cols

    me = lax.axis_index("sp")
    chip = lax.div(me, 2)
    core = lax.rem(me, 2)
    sibling = 2 * chip + (1 - core)

    def offset_of(idx):
        odd = lax.rem(idx, 2)
        return lax.rem(half_chip + odd + (2 * odd - 1) * lax.div(idx, 2), n_chip)

    def group_col(idx):
        dest = lax.rem(chip + offset_of(idx), n_chip)
        return pl.multiple_of((2 * dest + core) * cols, cols)

    def w_copy(w_ref, s, half):
        return pltpu.make_async_copy(
            w_ref.at[:, pl.ds(group_col(2 * s + half), cols)], pool.at[s, :, pl.ds(half * cols, cols)], wsem.at[s])

    def w_wait(s):
        pltpu.make_async_copy(pool.at[s], pool.at[s], wsem.at[s]).wait()

    def wo_copy(j):
        return pltpu.make_async_copy(wo.at[:, pl.ds(pl.multiple_of(j * wide, wide), wide)], pool.at[j], wosem)

    barrier = pltpu.get_barrier_semaphore()
    for off in sorted(range(1, n_dev), key=lambda off: -min(off, n_dev - off)):
        pl.semaphore_signal(barrier, inc=1, device_id={"sp": lax.rem(me + off, n_dev)}, device_id_type=MESH)

    my_rows = pl.ds(pl.multiple_of(core * tok, tok), tok)
    x_copy = pltpu.make_async_copy(x_hbm, xs.at[my_rows], xsem)
    x_copy.start()
    smalls = [pltpu.make_async_copy(a, b, insem.at[n]) for a, b, n in (
        (new_hbm, new_ref, 0), (qg_hbm, gains.at[0], 1), (kg_hbm, gains.at[1], 1), (pg_hbm, gains.at[2], 1))]
    w_copy(wv, 0, 0).start()
    w_copy(wv, 0, 1).start()
    for small in smalls:
        small.start()
    tab_a = pltpu.make_async_copy(tab_hbm.at[pl.ds(pl.multiple_of(chip * rows, rows), rows)], tab.at[pl.ds(0, rows)], tabsem)
    tab_b = pltpu.make_async_copy(tab_hbm.at[pl.ds(seq, PAD)], tab.at[pl.ds(rows, PAD)], tabsem)
    tab_a.start()
    tab_b.start()

    x_copy.wait()
    for s in range(1, n_step):
        w_copy(wv, s, 0).start()
        w_copy(wv, s, 1).start()

    own_rows = pl.ds(pl.multiple_of(chip * rows, rows), rows)

    def exchange(t, idx):
        dest = lax.rem(chip + offset_of(idx), n_chip)
        return pltpu.make_async_remote_copy(
            src_ref=send.at[t, idx], dst_ref=recv.at[t, own_rows], send_sem=a_s.at[t], recv_sem=a_r.at[t] if t else q_r.at[idx],
            device_id={"sp": 2 * dest + core}, device_id_type=MESH)

    def emit(t, idx, block):
        @pl.when(idx < n_chip - 1)
        def _():
            send[t, idx] = block[:rows]
            exchange(t, idx).start()

        @pl.when(idx == n_chip - 1)
        def _():
            recv[t, own_rows, :] = block[:rows]
            new[t] = block[rows:]

    def project(s):
        w_wait(s)
        return jnp.dot(xs[...], pool[s], preferred_element_type=F32)

    def half_exchange(idx, which):
        dest = lax.rem(chip + offset_of(idx), n_chip)
        at = pl.ds(pl.multiple_of(which * tok, tok), tok)
        return pltpu.make_async_remote_copy(
            src_ref=send.at[2, idx, at], dst_ref=recv.at[2, pl.ds(pl.multiple_of(chip * rows + which * tok, tok), tok)],
            send_sem=a_s.at[2], recv_sem=a_r.at[2], device_id={"sp": 2 * dest + core}, device_id_type=MESH)

    def half_project(which):
        at = pl.ds(pl.multiple_of(which * tok, tok), tok)
        res = jnp.dot(xs[at, :], pool[0], preferred_element_type=F32).astype(BF16)
        for idx in range(2):
            send[2, idx, at, :] = res[:, idx * cols:(idx + 1) * cols]

    w_wait(0)
    with jax.named_scope("v_first"):
        half_project(core)
    with jax.named_scope("barrier"):
        pl.semaphore_wait(barrier, n_dev - 1)
    x_send = pltpu.make_async_remote_copy(
        src_ref=xs.at[my_rows], dst_ref=xs.at[my_rows], send_sem=xs_s, recv_sem=xs_r, device_id={"sp": sibling}, device_id_type=MESH)
    x_send.start()
    for idx in range(2):
        half_exchange(idx, core).start()
    smalls[0].wait()
    pltpu.make_async_copy(gains, gains, insem.at[1]).wait()
    xs[pl.ds(rows, PAD), :] = jnp.broadcast_to(new_ref[...], (PAD, width))
    acc[...] = jnp.zeros_like(acc)
    with jax.named_scope("x_arrive"):
        x_send.wait_recv()

    def v_step(s, carry):
        res = project(s)
        w_copy(wk, s, 0).start()
        w_copy(wk, s, 1).start()
        for half in range(2):
            emit(2, 2 * s + half, res[:, half * cols:(half + 1) * cols].astype(BF16))
        return carry

    with jax.named_scope('v_proj'):
        lax.fori_loop(1, n_step, v_step, 0)
        half_project(1 - core)
        for idx in range(2):
            half_exchange(idx, 1 - core).start()
        w_copy(wk, 0, 0).start()
        w_copy(wk, 0, 1).start()
    pltpu.make_async_copy(tab, tab, tabsem).wait()

    lane = lax.broadcasted_iota(jnp.int32, (rows + PAD, HEAD_DIM), 1)
    first = lane < HEAD_DIM // 2

    def raw_step(t, i):
        s = lax.rem(i + 1, n_step)
        res = project(s)
        sq = jnp.zeros((rows + PAD, HEAD_DIM), F32)
        for half in range(2):
            part = res[:, half * cols:(half + 1) * cols]
            raw[2 * s + half] = part
            for h in range(heads):
                piece = part[:, h * HEAD_DIM:(h + 1) * HEAD_DIM]
                sq = sq + piece * piece
        @pl.when(i == 0)
        def _():
            ssq[t] = sq

        @pl.when(i > 0)
        def _():
            ssq[t] += sq

        return s

    def norm_and_send(t, g_ref):
        swap = pltpu.make_async_remote_copy(
            src_ref=ssq.at[t], dst_ref=ssq_in.at[t], send_sem=ss_s.at[t], recv_sem=ss_r.at[t],
            device_id={"sp": sibling}, device_id_type=MESH)
        swap.start()
        swap.wait_recv()
        total = jnp.sum(ssq[t] + ssq_in[t], axis=1, keepdims=True)
        scale = lax.rsqrt(total * (1.0 / width) + NORM_EPS)

        def one(n, carry):
            idx = n if t else n_chip - 1 - n
            g = g_ref[:, pl.ds(group_col(idx), cols)]
            table = tab[...]
            turned = pltpu.roll(table, HEAD_DIM // 2, 1)
            cos = jnp.where(first, table, turned)
            sin = jnp.where(first, -turned, table)
            parts = []
            for h in range(heads):
                at = slice(h * HEAD_DIM, (h + 1) * HEAD_DIM)
                val = raw[idx, :, at] * scale * g[:, at]
                parts.append((val * cos + pltpu.roll(val, HEAD_DIM // 2, 1) * sin).astype(BF16))
            emit(t, idx, jnp.concatenate(parts, axis=1))
            return carry

        lax.fori_loop(0, n_chip, one, 0)

    def k_step(i, carry):
        s = raw_step(1, i)
        w_copy(wq, s, 0).start()
        w_copy(wq, s, 1).start()
        return carry

    with jax.named_scope('k_proj'):
        lax.fori_loop(0, n_step, k_step, 0)
    with jax.named_scope('k_norm'):
        norm_and_send(1, gains.at[1])
    for j in range(n_step, n_wo):
        wo_copy(j).start()

    def q_step(i, carry):
        s = raw_step(0, i)
        wo_copy(s).start()
        return carry

    with jax.named_scope('q_proj'):
        lax.fori_loop(0, n_step, q_step, 0)
    with jax.named_scope('q_norm'):
        norm_and_send(0, gains.at[0])

    def whole(t):
        every = pl.ds(0, (n_chip - 1) * rows)
        return pltpu.make_async_remote_copy(
            src_ref=recv.at[t, every], dst_ref=recv.at[t, every], send_sem=a_s.at[t], recv_sem=a_r.at[t],
            device_id={"sp": sibling}, device_id_type=MESH)

    def fill_cache(t, cache):
        def one(b, carry):
            base = pl.multiple_of(b * rows, rows)
            block = recv[t, pl.ds(base, rows), :].astype(F32)
            for h in range(heads):
                stage[pl.ds(h, rows, stride=heads), :] = block[:, h * HEAD_DIM:(h + 1) * HEAD_DIM]
            cache[pl.ds(pl.multiple_of(heads * base, heads * rows), heads * rows), :] = stage[...].astype(BF16)
            return carry
        lax.fori_loop(0, n_chip, one, 0)
        last = new[t][0:1, :].astype(F32)
        rows_new = jnp.concatenate([last[:, h * HEAD_DIM:(h + 1) * HEAD_DIM] for h in range(heads)], axis=0)
        cache[pl.ds(heads * seq, heads), :] = rows_new.astype(BF16)

    with jax.named_scope("v_arrive"):
        whole(2).wait_recv()
    with jax.named_scope("v_cache"):
        fill_cache(2, vc_ref)
        for b in range(n_chip):
            for h in range(heads):
                vt[h, :, b * rows:(b + 1) * rows] = recv[2, b * rows:(b + 1) * rows, h * HEAD_DIM:(h + 1) * HEAD_DIM].astype(F32).T.astype(BF16)
    with jax.named_scope("k_arrive"):
        whole(1).wait_recv()
    with jax.named_scope("k_cache"):
        fill_cache(1, kc_ref)

    log_scale = HEAD_DIM ** -0.5 * math.log2(math.e)
    contract_last = (((1,), (1,)), ((), ()))

    for h in range(heads):
        at = slice(h * HEAD_DIM, (h + 1) * HEAD_DIM)
        qd, kd, vd = new[0][:, at], new[1][:, at], new[2][:, at]
        sc = lax.dot_general(qd, recv[1, :, at], contract_last, preferred_element_type=F32) * log_scale
        sn = jnp.sum(qd.astype(F32) * kd.astype(F32), axis=1, keepdims=True) * log_scale
        top = jnp.maximum(jnp.max(sc, axis=1, keepdims=True), sn)
        ex = jnp.exp2(sc - top)
        en = jnp.exp2(sn - top)
        inv = 1.0 / (jnp.sum(ex, axis=1, keepdims=True) + en)
        prob = (ex * inv).astype(BF16)
        prob_n = (en * inv).astype(BF16).astype(F32)
        od = jnp.dot(prob, recv[2, :, at], preferred_element_type=F32) + prob_n * vd.astype(F32)
        dsend[:, at] = od[0:1].astype(BF16).astype(F32)

    def d_copy(off, to):
        return pltpu.make_async_remote_copy(
            src_ref=dsend, dst_ref=dsum.at[2 * off + core], send_sem=d_s, recv_sem=d_r,
            device_id={"sp": to}, device_id_type=MESH)

    d_copy(0, sibling).start()
    for off in range(1, n_chip):
        for kk in range(2):
            d_copy(off, 2 * lax.rem(chip + off, n_chip) + kk).start()
    dsum[core] = dsend[...]

    def d_whole():
        every = pl.ds(0, n_dev - 1)
        return pltpu.make_async_remote_copy(
            src_ref=dsum.at[every], dst_ref=dsum.at[every], send_sem=d_s, recv_sem=d_r,
            device_id={"sp": sibling}, device_id_type=MESH)

    def o_copy(i, kk, to, off_o, near=0):
        return pltpu.make_async_remote_copy(
            src_ref=osend.at[i, pl.ds(pl.multiple_of(kk * tok, tok), tok)],
            dst_ref=orecv.at[off_o, pl.ds(0, tok), pl.ds(pl.multiple_of(core * cols, cols), cols)],
            send_sem=o_s.at[near], recv_sem=o_r.at[off_o], device_id={"sp": to}, device_id_type=MESH)

    def fold(block, op):
        return op(block.reshape(block.shape[0] // 8, 8, block.shape[1]), axis=0)

    def attend(i):
        idx = n_chip - 1 - i
        off_q = offset_of(idx)
        src = lax.rem(chip + n_chip - off_q, n_chip)
        off_o = lax.rem(n_chip - off_q, n_chip)

        @pl.when(i > 0)
        def _():
            with jax.named_scope("q_arrive"):
                exchange(0, idx).wait_recv()

        src_at = pl.ds(pl.multiple_of(src * rows, rows), rows)
        causal = lax.broadcasted_iota(jnp.int32, (rows, rows), 0) <= lax.broadcasted_iota(jnp.int32, (rows, rows), 1)
        blocks = [slice(kb * rows, (kb + 1) * rows) for kb in range(n_chip)]
        tops = []
        for h in range(heads):
            at = slice(h * HEAD_DIM, (h + 1) * HEAD_DIM)
            sc = lax.dot_general(recv[1, :, at], recv[0, src_at, at], contract_last, preferred_element_type=F32)
            s_ref[h] = sc
            top = jnp.full((8, rows), -jnp.inf, F32)
            for kb in range(n_chip):
                top = jnp.maximum(top, fold(sc[blocks[kb]], jnp.max) + jnp.where(kb < src, 0.0, -jnp.inf))
            tops.append(top)
        for h in range(heads):
            at = slice(h * HEAD_DIM, (h + 1) * HEAD_DIM)
            own = jnp.where(causal, s_ref[h, src_at, :], -jnp.inf)
            s_ref[h, src_at, :] = own
            top = jnp.max(jnp.maximum(tops[h], fold(own, jnp.max)), axis=0, keepdims=True) * log_scale
            total = jnp.zeros((8, rows), F32)
            for kb in range(n_chip):
                ex = jnp.exp2(s_ref[h, blocks[kb], :] * log_scale + (jnp.where(kb <= src, 0.0, -jnp.inf) - top))
                s_ref[h, blocks[kb], :] = ex
                total = total + fold(ex, jnp.sum)
            inv = 1.0 / jnp.sum(total, axis=0, keepdims=True)
            for kb in range(n_chip):
                p_ref[h, blocks[kb], :] = (s_ref[h, blocks[kb], :] * inv).astype(BF16)
            osend[i, :, at] = jnp.dot(vt[h], p_ref[h], preferred_element_type=F32).T.astype(BF16)

        @pl.when(i > 0)
        def _():
            for kk in range(2):
                o_copy(i, kk, 2 * src + kk, off_o).start()

        @pl.when(i == 0)
        def _():
            o_copy(i, 1 - core, sibling, off_o, 1).start()
            orecv[0, pl.ds(0, tok), pl.ds(pl.multiple_of(core * cols, cols), cols)] = osend[0, my_rows, :]

    zero_half = jnp.zeros((8, cols), BF16)

    def gather(i):
        off_o = lax.rem(n_chip - offset_of(n_chip - 1 - i), n_chip)
        src = lax.rem(chip + n_chip - off_o, n_chip)

        def arrived(span):
            at = (off_o, pl.ds(0, tok), span)
            pltpu.make_async_remote_copy(
                src_ref=orecv.at[at], dst_ref=orecv.at[at], send_sem=o_s.at[0], recv_sem=o_r.at[off_o],
                device_id={"sp": sibling}, device_id_type=MESH).wait_recv()

        @pl.when(i == 0)
        def _():
            d_whole().wait_recv()
            arrived(pl.ds(pl.multiple_of((1 - core) * cols, cols), cols))

        @pl.when(i > 0)
        def _():
            with jax.named_scope("o_arrive"):
                arrived(pl.ds(0, wide))

        d0 = jnp.broadcast_to(dsum[2 * off_o].astype(BF16), (8, cols))
        d1 = jnp.broadcast_to(dsum[2 * off_o + 1].astype(BF16), (8, cols))
        orecv[off_o, pl.ds(tok, PAD), :] = jnp.concatenate(
            [jnp.concatenate([d0, zero_half], axis=1), jnp.concatenate([zero_half, d1], axis=1)], axis=0)
        k_at = pl.ds(pl.multiple_of(src * wide, wide), wide)
        lhs = orecv[off_o]
        for j in range(n_wo):
            res = jnp.dot(lhs, pool[j, k_at, :], preferred_element_type=F32)
            parts = res[tok:tok + 8].astype(BF16).astype(F32) + res[tok + 8:].astype(BF16).astype(F32)
            n_at = slice(j * wide, (j + 1) * wide)
            acc[pl.ds(0, tok), n_at] += res[:tok]
            acc[pl.ds(tok, 8), n_at] += parts

    def drain_early():
        x_send.wait_send()
        for t in range(2):
            pltpu.make_async_remote_copy(
                src_ref=ssq.at[t], dst_ref=ssq_in.at[t], send_sem=ss_s.at[t], recv_sem=ss_r.at[t],
                device_id={"sp": sibling}, device_id_type=MESH).wait_send()

        for t in range(3):
            whole(t).wait_send()
        d_whole().wait_send()

    def both(i, carry):
        @pl.when(i < n_chip)
        def _():
            with jax.named_scope("attend"):
                attend(i)

        @pl.when(i == LAG)
        def _():
            pltpu.make_async_copy(pool, pool, wosem).wait()
            drain_early()

        @pl.when(i >= LAG)
        def _():
            with jax.named_scope("gather"):
                gather(i - LAG)
        return carry

    lax.fori_loop(0, n_chip + LAG, both, 0)

    def finish(r):
        r_at = pl.ds(r * PAD, PAD)
        val = acc[r_at, :]
        scale = lax.rsqrt(jnp.sum(val * val, axis=1, keepdims=True) * (1.0 / width) + NORM_EPS)
        x_at = pl.ds(pl.multiple_of(core * tok + r * PAD, PAD), PAD)
        outp_ref[r_at, :] = (xs[x_at, :].astype(F32) + val * scale * gains[2]).astype(BF16)

    with jax.named_scope("finish"):
        for r in range(tok // PAD):
            finish(r)
        val = acc[pl.ds(tok, 8), :]
        scale = lax.rsqrt(jnp.sum(val * val, axis=1, keepdims=True) * (1.0 / width) + NORM_EPS)
        outd_ref[...] = (new_ref[...].astype(F32) + (val * scale * gains[2])[0:1]).astype(BF16)

    o_copy(0, 1 - core, sibling, 0, 1).wait_send()
    far = osend.at[pl.ds(1, n_chip - 1)]
    pltpu.make_async_remote_copy(
        src_ref=far, dst_ref=far, send_sem=o_s.at[0], recv_sem=o_r.at[0],
        device_id={"sp": sibling}, device_id_type=MESH).wait_send()


def hand_over(outp_in, kc_in, vc_in, outd_in, outp, kc, vc, outd, sem):
    outs = [pltpu.make_async_copy(a, b, sem.at[n]) for n, (a, b) in enumerate(
        ((outp_in, outp), (kc_in, kc.reshape(kc_in.shape)), (vc_in, vc.reshape(vc_in.shape)), (outd_in, outd)))]
    for one in outs:
        one.start()
    for one in outs:
        one.wait()


def solution(mesh):
    n_dev = mesh.shape["sp"]

    def device_step(prompt_blk, w_q, w_k, w_v, w_o, q_norm_w, k_norm_w, post_norm_w, new_rows):
        _, tok, width = prompt_blk.shape
        n_chip = n_dev // 2
        rows, seq, cols = 2 * tok, tok * n_dev, width // n_dev
        heads = cols // HEAD_DIM
        wide = 2 * cols
        n_wo = width // wide
        table = jnp.asarray(rope_table(seq))
        hbm = pl.BlockSpec(memory_space=pltpu.HBM)
        vmem = pl.BlockSpec(memory_space=pltpu.VMEM)
        dma = pltpu.SemaphoreType.DMA
        cache_shape = jax.ShapeDtypeStruct((heads * (seq + 1), HEAD_DIM), BF16)

        def keep(value):
            return pltpu.with_memory_space_constraint(value, pltpu.HBM)

        outp, kc, vc, outd = pl.pallas_call(
            functools.partial(kernel, n_dev),
            out_shape=(jax.ShapeDtypeStruct((tok, width), BF16), cache_shape, cache_shape, jax.ShapeDtypeStruct((1, width), BF16)),
            in_specs=[hbm] * 10,
            out_specs=(vmem,) * 4,
            scratch_shapes=[
                pltpu.VMEM((1, width), BF16),
                pltpu.VMEM((3, 1, width), F32),
                pltpu.VMEM((rows + PAD, width), BF16),
                pltpu.VMEM((n_wo, width, wide), BF16),
                pltpu.VMEM((rows + PAD, HEAD_DIM), F32),
                pltpu.VMEM((n_chip, rows + PAD, cols), F32),
                pltpu.VMEM((2, rows + PAD, HEAD_DIM), F32),
                pltpu.VMEM((2, rows + PAD, HEAD_DIM), F32),
                pltpu.VMEM((3, n_chip, rows, cols), BF16),
                pltpu.VMEM((3, seq, cols), BF16),
                pltpu.VMEM((3, PAD, cols), BF16),
                pltpu.VMEM((heads, seq, rows), F32),
                pltpu.VMEM((heads, seq, rows), BF16),
                pltpu.VMEM((heads, HEAD_DIM, seq), BF16),
                pltpu.VMEM((n_chip, rows, cols), BF16),
                pltpu.VMEM((n_chip, tok + PAD, wide), BF16),
                pltpu.VMEM((1, cols), F32),
                pltpu.VMEM((n_dev, 1, cols), F32),
                pltpu.VMEM((tok + 8, width), F32),
                pltpu.VMEM((heads * rows, HEAD_DIM), F32),
                dma(()), dma((2,)), dma((n_chip // 2,)), dma(()), dma(()),
                dma(()), dma(()), dma((2,)), dma((2,)),
                dma((3,)), dma((3,)), dma((n_chip,)),
                dma(()), dma(()),
                dma((2,)), dma((n_chip,)),
            ],
            compiler_params=pltpu.CompilerParams(collective_id=0, has_side_effects=True, vmem_limit_bytes=VMEM_MIB * 1024 * 1024),
        )(keep(prompt_blk[0]), keep(new_rows), w_q, w_k, w_v, w_o, keep(q_norm_w[None]), keep(k_norm_w[None]), keep(post_norm_w[None]), keep(table))
        shape = (seq + 1, heads, HEAD_DIM)
        outs = pl.pallas_call(
            hand_over,
            out_shape=(jax.ShapeDtypeStruct((tok, width), BF16), jax.ShapeDtypeStruct(shape, BF16),
                       jax.ShapeDtypeStruct(shape, BF16), jax.ShapeDtypeStruct((1, width), BF16)),
            in_specs=[vmem] * 4,
            out_specs=(hbm,) * 4,
            scratch_shapes=[dma((4,))],
            compiler_params=pltpu.CompilerParams(vmem_limit_bytes=8 * 1024 * 1024),
        )(outp, kc, vc, outd)
        return outs[0][None], outs[1][None], outs[2][None], outs[3]

    replicated = P()
    return jax.shard_map(
        device_step, mesh=mesh,
        in_specs=(P("dp", "sp", None), replicated, replicated, replicated, replicated, replicated, replicated, replicated, P("dp", None)),
        out_specs=(P("dp", "sp", None), P("dp", None, "sp", None), P("dp", None, "sp", None), P("dp", None)),
        check_vma=False)
```

```python
import functools
import math

import jax
import jax.numpy as jnp
import numpy as np
from jax import lax
from jax.experimental import pallas as pl
from jax.experimental.pallas import tpu as pltpu
from jax.sharding import PartitionSpec as P

HEAD_DIM = 128
ROPE_THETA = 500000.0
NORM_EPS = 1e-6
PAD = 16
VMEM_MIB = 50
LAG = 6
MASKED = -1e30
F32 = jnp.float32
BF16 = jnp.bfloat16
MESH = pl.DeviceIdType.MESH


def rope_table(seq_len):
    half = HEAD_DIM // 2
    inv_freq = np.power(np.float32(ROPE_THETA), -np.arange(0, HEAD_DIM, 2).astype(np.float32) / np.float32(HEAD_DIM)).astype(np.float32)
    pos = np.minimum(np.arange(seq_len + PAD), seq_len).astype(np.float32)
    angles = (pos[:, None] * inv_freq[None, :half]).astype(np.float32)
    return np.concatenate([np.cos(angles), np.sin(angles)], axis=-1).astype(np.float32)


def kernel(n_dev, x_hbm, new_hbm, wq, wk, wv, wo, qg_hbm, kg_hbm, pg_hbm, tab_hbm,
           outp_ref, kc_ref, vc_ref, outd_ref,
           new_ref, gains,
           xs, pool, tab, raw, ssq, ssq_in, send, recv, new, s_ref, p_ref, vt, osend, orecv, dsend, dsum, acc, stage,
           xsem, insem, wsem, wosem, tabsem, xs_s, xs_r, ss_s, ss_r, a_s, a_r, q_r, d_s, d_r, o_s, o_r):
    tok = x_hbm.shape[0]
    width = x_hbm.shape[1]
    rows = 2 * tok
    n_chip = n_dev // 2
    half_chip = n_chip // 2
    cols = width // n_dev
    heads = cols // HEAD_DIM
    seq = tok * n_dev
    n_step = n_chip // 2
    n_wo = pool.shape[0]
    wide = 2 * cols

    me = lax.axis_index("sp")
    chip = lax.div(me, 2)
    core = lax.rem(me, 2)
    sibling = 2 * chip + (1 - core)

    def offset_of(idx):
        odd = lax.rem(idx, 2)
        return lax.rem(half_chip + odd + (2 * odd - 1) * lax.div(idx, 2), n_chip)

    def group_col(idx):
        dest = lax.rem(chip + offset_of(idx), n_chip)
        return pl.multiple_of((2 * dest + core) * cols, cols)

    def w_copy(w_ref, s, half):
        return pltpu.make_async_copy(
            w_ref.at[:, pl.ds(group_col(2 * s + half), cols)], pool.at[s, :, pl.ds(half * cols, cols)], wsem.at[s])

    def w_wait(s):
        pltpu.make_async_copy(pool.at[s], pool.at[s], wsem.at[s]).wait()

    def wo_copy(j):
        return pltpu.make_async_copy(wo.at[:, pl.ds(pl.multiple_of(j * wide, wide), wide)], pool.at[j], wosem)

    my_rows = pl.ds(pl.multiple_of(core * tok, tok), tok)
    x_copy = pltpu.make_async_copy(x_hbm, xs.at[my_rows], xsem)
    x_copy.start()

    barrier = pltpu.get_barrier_semaphore()
    for off in sorted(range(1, n_dev), key=lambda off: -min(off, n_dev - off)):
        pl.semaphore_signal(barrier, inc=1, device_id={"sp": lax.rem(me + off, n_dev)}, device_id_type=MESH)

    smalls = [pltpu.make_async_copy(a, b, insem.at[n]) for a, b, n in (
        (new_hbm, new_ref, 0), (qg_hbm, gains.at[0], 1), (kg_hbm, gains.at[1], 1), (pg_hbm, gains.at[2], 1))]
    w_copy(wv, 0, 0).start()
    w_copy(wv, 0, 1).start()
    for small in smalls:
        small.start()
    tab_a = pltpu.make_async_copy(tab_hbm.at[pl.ds(pl.multiple_of(chip * rows, rows), rows)], tab.at[pl.ds(0, rows)], tabsem)
    tab_b = pltpu.make_async_copy(tab_hbm.at[pl.ds(seq, PAD)], tab.at[pl.ds(rows, PAD)], tabsem)
    tab_a.start()
    tab_b.start()

    x_copy.wait()
    for s in range(1, n_step):
        w_copy(wv, s, 0).start()
        w_copy(wv, s, 1).start()

    own_rows = pl.ds(pl.multiple_of(chip * rows, rows), rows)

    def exchange(t, idx):
        dest = lax.rem(chip + offset_of(idx), n_chip)
        return pltpu.make_async_remote_copy(
            src_ref=send.at[t, idx], dst_ref=recv.at[t, own_rows], send_sem=a_s.at[t], recv_sem=a_r.at[t] if t else q_r.at[idx],
            device_id={"sp": 2 * dest + core}, device_id_type=MESH)

    def emit(t, idx, block):
        @pl.when(idx < n_chip - 1)
        def _():
            send[t, idx] = block[:rows]
            exchange(t, idx).start()

        @pl.when(idx == n_chip - 1)
        def _():
            recv[t, own_rows, :] = block[:rows]
            new[t] = block[rows:]

    def project(s):
        w_wait(s)
        return jnp.dot(xs[...], pool[s], preferred_element_type=F32)

    def half_exchange(idx, which):
        dest = lax.rem(chip + offset_of(idx), n_chip)
        at = pl.ds(pl.multiple_of(which * tok, tok), tok)
        return pltpu.make_async_remote_copy(
            src_ref=send.at[2, idx, at], dst_ref=recv.at[2, pl.ds(pl.multiple_of(chip * rows + which * tok, tok), tok)],
            send_sem=a_s.at[2], recv_sem=a_r.at[2], device_id={"sp": 2 * dest + core}, device_id_type=MESH)

    def half_project(which):
        at = pl.ds(pl.multiple_of(which * tok, tok), tok)
        res = jnp.dot(xs[at, :], pool[0], preferred_element_type=F32).astype(BF16)
        for idx in range(2):
            send[2, idx, at, :] = res[:, idx * cols:(idx + 1) * cols]

    w_wait(0)
    with jax.named_scope("v_first"):
        half_project(core)
    with jax.named_scope("barrier"):
        pl.semaphore_wait(barrier, n_dev - 1)
    x_send = pltpu.make_async_remote_copy(
        src_ref=xs.at[my_rows], dst_ref=xs.at[my_rows], send_sem=xs_s, recv_sem=xs_r, device_id={"sp": sibling}, device_id_type=MESH)
    x_send.start()
    for idx in range(2):
        half_exchange(idx, core).start()
    smalls[0].wait()
    pltpu.make_async_copy(gains, gains, insem.at[1]).wait()
    xs[pl.ds(rows, PAD), :] = jnp.broadcast_to(new_ref[...], (PAD, width))
    acc[...] = jnp.zeros_like(acc)
    with jax.named_scope("x_arrive"):
        x_send.wait_recv()

    def v_step(s, carry):
        res = project(s)
        w_copy(wk, s, 0).start()
        w_copy(wk, s, 1).start()
        for half in range(2):
            emit(2, 2 * s + half, res[:, half * cols:(half + 1) * cols].astype(BF16))
        return carry

    with jax.named_scope('v_proj'):
        lax.fori_loop(1, n_step, v_step, 0)
        half_project(1 - core)
        for idx in range(2):
            half_exchange(idx, 1 - core).start()
        w_copy(wk, 0, 0).start()
        w_copy(wk, 0, 1).start()
    pltpu.make_async_copy(tab, tab, tabsem).wait()

    lane = lax.broadcasted_iota(jnp.int32, (rows + PAD, HEAD_DIM), 1)
    first = lane < HEAD_DIM // 2

    def raw_step(t, i):
        s = lax.rem(i + 1, n_step)
        res = project(s)
        sq = jnp.zeros((rows + PAD, HEAD_DIM), F32)
        for half in range(2):
            part = res[:, half * cols:(half + 1) * cols]
            raw[2 * s + half] = part
            for h in range(heads):
                piece = part[:, h * HEAD_DIM:(h + 1) * HEAD_DIM]
                sq = sq + piece * piece
        @pl.when(i == 0)
        def _():
            ssq[t] = sq

        @pl.when(i > 0)
        def _():
            ssq[t] += sq

        return s

    def norm_and_send(t, g_ref):
        swap = pltpu.make_async_remote_copy(
            src_ref=ssq.at[t], dst_ref=ssq_in.at[t], send_sem=ss_s.at[t], recv_sem=ss_r.at[t],
            device_id={"sp": sibling}, device_id_type=MESH)
        swap.start()
        swap.wait_recv()
        total = jnp.sum(ssq[t] + ssq_in[t], axis=1, keepdims=True)
        scale = lax.rsqrt(total * (1.0 / width) + NORM_EPS)

        def one(n, carry):
            idx = n if t else n_chip - 1 - n
            g = g_ref[:, pl.ds(group_col(idx), cols)]
            table = tab[...]
            turned = pltpu.roll(table, HEAD_DIM // 2, 1)
            cos = jnp.where(first, table, turned)
            sin = jnp.where(first, -turned, table)
            parts = []
            for h in range(heads):
                at = slice(h * HEAD_DIM, (h + 1) * HEAD_DIM)
                val = raw[idx, :, at] * scale * g[:, at]
                parts.append((val * cos + pltpu.roll(val, HEAD_DIM // 2, 1) * sin).astype(BF16))
            emit(t, idx, jnp.concatenate(parts, axis=1))
            return carry

        lax.fori_loop(0, n_chip, one, 0)

    def k_step(i, carry):
        s = raw_step(1, i)
        w_copy(wq, s, 0).start()
        w_copy(wq, s, 1).start()
        return carry

    with jax.named_scope('k_proj'):
        lax.fori_loop(0, n_step, k_step, 0)
    with jax.named_scope('k_norm'):
        norm_and_send(1, gains.at[1])
    for j in range(n_step, n_wo):
        wo_copy(j).start()

    def q_step(i, carry):
        s = raw_step(0, i)
        wo_copy(s).start()
        return carry

    with jax.named_scope('q_proj'):
        lax.fori_loop(0, n_step, q_step, 0)
    with jax.named_scope('q_norm'):
        norm_and_send(0, gains.at[0])

    def whole(t):
        every = pl.ds(0, (n_chip - 1) * rows)
        return pltpu.make_async_remote_copy(
            src_ref=recv.at[t, every], dst_ref=recv.at[t, every], send_sem=a_s.at[t], recv_sem=a_r.at[t],
            device_id={"sp": sibling}, device_id_type=MESH)

    def fill_cache(t, cache):
        def one(b, carry):
            base = pl.multiple_of(b * rows, rows)
            block = recv[t, pl.ds(base, rows), :].astype(F32)
            for h in range(heads):
                stage[pl.ds(h, rows, stride=heads), :] = block[:, h * HEAD_DIM:(h + 1) * HEAD_DIM]
            cache[pl.ds(pl.multiple_of(heads * base, heads * rows), heads * rows), :] = stage[...].astype(BF16)
            return carry
        lax.fori_loop(0, n_chip, one, 0)
        last = new[t][0:1, :].astype(F32)
        rows_new = jnp.concatenate([last[:, h * HEAD_DIM:(h + 1) * HEAD_DIM] for h in range(heads)], axis=0)
        cache[pl.ds(heads * seq, heads), :] = rows_new.astype(BF16)

    with jax.named_scope("v_arrive"):
        whole(2).wait_recv()
    with jax.named_scope("v_cache"):
        fill_cache(2, vc_ref)
        for b in range(n_chip):
            for h in range(heads):
                vt[h, :, b * rows:(b + 1) * rows] = recv[2, b * rows:(b + 1) * rows, h * HEAD_DIM:(h + 1) * HEAD_DIM].astype(F32).T.astype(BF16)
    with jax.named_scope("k_arrive"):
        whole(1).wait_recv()
    with jax.named_scope("k_cache"):
        fill_cache(1, kc_ref)

    log_scale = HEAD_DIM ** -0.5 * math.log2(math.e)
    contract_last = (((1,), (1,)), ((), ()))

    for h in range(heads):
        at = slice(h * HEAD_DIM, (h + 1) * HEAD_DIM)
        qd, kd, vd = new[0][:, at], new[1][:, at], new[2][:, at]
        sc = lax.dot_general(qd, recv[1, :, at], contract_last, preferred_element_type=F32) * log_scale
        sn = jnp.sum(qd.astype(F32) * kd.astype(F32), axis=1, keepdims=True) * log_scale
        top = jnp.maximum(jnp.max(sc, axis=1, keepdims=True), sn)
        ex = jnp.exp2(sc - top)
        en = jnp.exp2(sn - top)
        inv = 1.0 / (jnp.sum(ex, axis=1, keepdims=True) + en)
        prob = (ex * inv).astype(BF16)
        prob_n = (en * inv).astype(BF16).astype(F32)
        od = jnp.dot(prob, recv[2, :, at], preferred_element_type=F32) + prob_n * vd.astype(F32)
        dsend[:, at] = od[0:1].astype(BF16).astype(F32)

    def d_copy(off, to):
        return pltpu.make_async_remote_copy(
            src_ref=dsend, dst_ref=dsum.at[2 * off + core], send_sem=d_s, recv_sem=d_r,
            device_id={"sp": to}, device_id_type=MESH)

    d_copy(0, sibling).start()
    for off in range(1, n_chip):
        for kk in range(2):
            d_copy(off, 2 * lax.rem(chip + off, n_chip) + kk).start()
    dsum[core] = dsend[...]

    def d_whole():
        every = pl.ds(0, n_dev - 1)
        return pltpu.make_async_remote_copy(
            src_ref=dsum.at[every], dst_ref=dsum.at[every], send_sem=d_s, recv_sem=d_r,
            device_id={"sp": sibling}, device_id_type=MESH)

    def o_copy(i, kk, to, off_o, near=0):
        return pltpu.make_async_remote_copy(
            src_ref=osend.at[i, pl.ds(pl.multiple_of(kk * tok, tok), tok)],
            dst_ref=orecv.at[off_o, pl.ds(0, tok), pl.ds(pl.multiple_of(core * cols, cols), cols)],
            send_sem=o_s.at[near], recv_sem=o_r.at[off_o], device_id={"sp": to}, device_id_type=MESH)

    def fold(block, op):
        return op(block.reshape(block.shape[0] // 8, 8, block.shape[1]), axis=0)

    def attend(i):
        idx = n_chip - 1 - i
        off_q = offset_of(idx)
        src = lax.rem(chip + n_chip - off_q, n_chip)
        off_o = lax.rem(n_chip - off_q, n_chip)

        @pl.when(i > 0)
        def _():
            with jax.named_scope("q_arrive"):
                exchange(0, idx).wait_recv()

        src_at = pl.ds(pl.multiple_of(src * rows, rows), rows)
        causal = lax.broadcasted_iota(jnp.int32, (rows, rows), 0) <= lax.broadcasted_iota(jnp.int32, (rows, rows), 1)
        blocks = [slice(kb * rows, (kb + 1) * rows) for kb in range(n_chip)]
        tops = []
        for h in range(heads):
            at = slice(h * HEAD_DIM, (h + 1) * HEAD_DIM)
            sc = lax.dot_general(recv[1, :, at], recv[0, src_at, at], contract_last, preferred_element_type=F32)
            s_ref[h] = sc
            top = jnp.full((8, rows), -jnp.inf, F32)
            for kb in range(n_chip):
                top = jnp.maximum(top, fold(sc[blocks[kb]], jnp.max) + jnp.where(kb < src, 0.0, -jnp.inf))
            tops.append(top)
        for h in range(heads):
            at = slice(h * HEAD_DIM, (h + 1) * HEAD_DIM)
            own = jnp.where(causal, s_ref[h, src_at, :], -jnp.inf)
            s_ref[h, src_at, :] = own
            top = jnp.max(jnp.maximum(tops[h], fold(own, jnp.max)), axis=0, keepdims=True) * log_scale
            total = jnp.zeros((8, rows), F32)
            for kb in range(n_chip):
                ex = jnp.exp2(s_ref[h, blocks[kb], :] * log_scale + (jnp.where(kb <= src, 0.0, -jnp.inf) - top))
                s_ref[h, blocks[kb], :] = ex
                total = total + fold(ex, jnp.sum)
            inv = 1.0 / jnp.sum(total, axis=0, keepdims=True)
            for kb in range(n_chip):
                p_ref[h, blocks[kb], :] = (s_ref[h, blocks[kb], :] * inv).astype(BF16)
            osend[i, :, at] = jnp.dot(vt[h], p_ref[h], preferred_element_type=F32).T.astype(BF16)

        @pl.when(i > 0)
        def _():
            for kk in range(2):
                o_copy(i, kk, 2 * src + kk, off_o).start()

        @pl.when(i == 0)
        def _():
            o_copy(i, 1 - core, sibling, off_o, 1).start()
            orecv[0, pl.ds(0, tok), pl.ds(pl.multiple_of(core * cols, cols), cols)] = osend[0, my_rows, :]

    zero_half = jnp.zeros((8, cols), BF16)

    def gather(i):
        off_o = lax.rem(n_chip - offset_of(n_chip - 1 - i), n_chip)
        src = lax.rem(chip + n_chip - off_o, n_chip)

        def arrived(span):
            at = (off_o, pl.ds(0, tok), span)
            pltpu.make_async_remote_copy(
                src_ref=orecv.at[at], dst_ref=orecv.at[at], send_sem=o_s.at[0], recv_sem=o_r.at[off_o],
                device_id={"sp": sibling}, device_id_type=MESH).wait_recv()

        @pl.when(i == 0)
        def _():
            d_whole().wait_recv()
            arrived(pl.ds(pl.multiple_of((1 - core) * cols, cols), cols))

        @pl.when(i > 0)
        def _():
            with jax.named_scope("o_arrive"):
                arrived(pl.ds(0, wide))

        d0 = jnp.broadcast_to(dsum[2 * off_o].astype(BF16), (8, cols))
        d1 = jnp.broadcast_to(dsum[2 * off_o + 1].astype(BF16), (8, cols))
        orecv[off_o, pl.ds(tok, PAD), :] = jnp.concatenate(
            [jnp.concatenate([d0, zero_half], axis=1), jnp.concatenate([zero_half, d1], axis=1)], axis=0)
        k_at = pl.ds(pl.multiple_of(src * wide, wide), wide)
        lhs = orecv[off_o]
        for j in range(n_wo):
            res = jnp.dot(lhs, pool[j, k_at, :], preferred_element_type=F32)
            parts = res[tok:tok + 8].astype(BF16).astype(F32) + res[tok + 8:].astype(BF16).astype(F32)
            n_at = slice(j * wide, (j + 1) * wide)
            acc[pl.ds(0, tok), n_at] += res[:tok]
            acc[pl.ds(tok, 8), n_at] += parts

    def drain_early():
        x_send.wait_send()
        for t in range(2):
            pltpu.make_async_remote_copy(
                src_ref=ssq.at[t], dst_ref=ssq_in.at[t], send_sem=ss_s.at[t], recv_sem=ss_r.at[t],
                device_id={"sp": sibling}, device_id_type=MESH).wait_send()

        for t in range(3):
            whole(t).wait_send()
        d_whole().wait_send()

    def both(i, carry):
        @pl.when(i < n_chip)
        def _():
            with jax.named_scope("attend"):
                attend(i)

        @pl.when(i == LAG)
        def _():
            pltpu.make_async_copy(pool, pool, wosem).wait()
            drain_early()

        @pl.when(i >= LAG)
        def _():
            with jax.named_scope("gather"):
                gather(i - LAG)
        return carry

    lax.fori_loop(0, n_chip + LAG, both, 0)

    def finish(r):
        r_at = pl.ds(r * PAD, PAD)
        val = acc[r_at, :]
        scale = lax.rsqrt(jnp.sum(val * val, axis=1, keepdims=True) * (1.0 / width) + NORM_EPS)
        x_at = pl.ds(pl.multiple_of(core * tok + r * PAD, PAD), PAD)
        outp_ref[r_at, :] = (xs[x_at, :].astype(F32) + val * scale * gains[2]).astype(BF16)

    with jax.named_scope("finish"):
        for r in range(tok // PAD):
            finish(r)
        val = acc[pl.ds(tok, 8), :]
        scale = lax.rsqrt(jnp.sum(val * val, axis=1, keepdims=True) * (1.0 / width) + NORM_EPS)
        outd_ref[...] = (new_ref[...].astype(F32) + (val * scale * gains[2])[0:1]).astype(BF16)

    o_copy(0, 1 - core, sibling, 0, 1).wait_send()
    far = osend.at[pl.ds(1, n_chip - 1)]
    pltpu.make_async_remote_copy(
        src_ref=far, dst_ref=far, send_sem=o_s.at[0], recv_sem=o_r.at[0],
        device_id={"sp": sibling}, device_id_type=MESH).wait_send()


def hand_over(outp_in, kc_in, vc_in, outd_in, outp, kc, vc, outd, sem):
    outs = [pltpu.make_async_copy(a, b, sem.at[n]) for n, (a, b) in enumerate(
        ((outp_in, outp), (kc_in, kc.reshape(kc_in.shape)), (vc_in, vc.reshape(vc_in.shape)), (outd_in, outd)))]
    for one in outs:
        one.start()
    for one in outs:
        one.wait()


def solution(mesh):
    n_dev = mesh.shape["sp"]

    def device_step(prompt_blk, w_q, w_k, w_v, w_o, q_norm_w, k_norm_w, post_norm_w, new_rows):
        _, tok, width = prompt_blk.shape
        n_chip = n_dev // 2
        rows, seq, cols = 2 * tok, tok * n_dev, width // n_dev
        heads = cols // HEAD_DIM
        wide = 2 * cols
        n_wo = width // wide
        table = jnp.asarray(rope_table(seq))
        hbm = pl.BlockSpec(memory_space=pltpu.HBM)
        vmem = pl.BlockSpec(memory_space=pltpu.VMEM)
        dma = pltpu.SemaphoreType.DMA
        cache_shape = jax.ShapeDtypeStruct((heads * (seq + 1), HEAD_DIM), BF16)

        def keep(value):
            return pltpu.with_memory_space_constraint(value, pltpu.HBM)

        outp, kc, vc, outd = pl.pallas_call(
            functools.partial(kernel, n_dev),
            out_shape=(jax.ShapeDtypeStruct((tok, width), BF16), cache_shape, cache_shape, jax.ShapeDtypeStruct((1, width), BF16)),
            in_specs=[hbm] * 10,
            out_specs=(vmem,) * 4,
            scratch_shapes=[
                pltpu.VMEM((1, width), BF16),
                pltpu.VMEM((3, 1, width), F32),
                pltpu.VMEM((rows + PAD, width), BF16),
                pltpu.VMEM((n_wo, width, wide), BF16),
                pltpu.VMEM((rows + PAD, HEAD_DIM), F32),
                pltpu.VMEM((n_chip, rows + PAD, cols), F32),
                pltpu.VMEM((2, rows + PAD, HEAD_DIM), F32),
                pltpu.VMEM((2, rows + PAD, HEAD_DIM), F32),
                pltpu.VMEM((3, n_chip, rows, cols), BF16),
                pltpu.VMEM((3, seq, cols), BF16),
                pltpu.VMEM((3, PAD, cols), BF16),
                pltpu.VMEM((heads, seq, rows), F32),
                pltpu.VMEM((heads, seq, rows), BF16),
                pltpu.VMEM((heads, HEAD_DIM, seq), BF16),
                pltpu.VMEM((n_chip, rows, cols), BF16),
                pltpu.VMEM((n_chip, tok + PAD, wide), BF16),
                pltpu.VMEM((1, cols), F32),
                pltpu.VMEM((n_dev, 1, cols), F32),
                pltpu.VMEM((tok + 8, width), F32),
                pltpu.VMEM((heads * rows, HEAD_DIM), F32),
                dma(()), dma((2,)), dma((n_chip // 2,)), dma(()), dma(()),
                dma(()), dma(()), dma((2,)), dma((2,)),
                dma((3,)), dma((3,)), dma((n_chip,)),
                dma(()), dma(()),
                dma((2,)), dma((n_chip,)),
            ],
            compiler_params=pltpu.CompilerParams(collective_id=0, has_side_effects=True, vmem_limit_bytes=VMEM_MIB * 1024 * 1024),
        )(keep(prompt_blk[0]), keep(new_rows), w_q, w_k, w_v, w_o, keep(q_norm_w[None]), keep(k_norm_w[None]), keep(post_norm_w[None]), keep(table))
        shape = (seq + 1, heads, HEAD_DIM)
        outs = pl.pallas_call(
            hand_over,
            out_shape=(jax.ShapeDtypeStruct((tok, width), BF16), jax.ShapeDtypeStruct(shape, BF16),
                       jax.ShapeDtypeStruct(shape, BF16), jax.ShapeDtypeStruct((1, width), BF16)),
            in_specs=[vmem] * 4,
            out_specs=(hbm,) * 4,
            scratch_shapes=[dma((4,))],
            compiler_params=pltpu.CompilerParams(vmem_limit_bytes=8 * 1024 * 1024),
        )(outp, kc, vc, outd)
        return outs[0][None], outs[1][None], outs[2][None], outs[3]

    replicated = P()
    return jax.shard_map(
        device_step, mesh=mesh,
        in_specs=(P("dp", "sp", None), replicated, replicated, replicated, replicated, replicated, replicated, replicated, P("dp", None)),
        out_specs=(P("dp", "sp", None), P("dp", None, "sp", None), P("dp", None, "sp", None), P("dp", None)),
        check_vma=False)
```
